32 devices in a mesh: groups: 2 (over y), expert: 4 (over x, core), cuts: 4 (over z).
Axes of the slice: x: 2, y: 2, z: 4, core: 2. Of those that a mesh axis runs over, the one named last changes fastest.
Arguments:
- tokens: bfloat16 [4096, 2048], P(('groups', 'expert')), parts along dimension 0, may hold values from -6 to 6
- route: int32 [4096, 1], P(('groups', 'expert')), parts along dimension 0, may hold values from 0 to 3; in each aligned block of 512 rows (0 to 511, 512 to 1023, ...) at most 192 rows name the same one
- gate_prob: float32 [4096], P(('groups', 'expert')), parts along dimension 0, may hold values from 0.2 to 1
- norm_gain: float32 [2048], replicated, may hold values from 0.5 to 1.5
- dense_in: bfloat16 [2048, 8192], P('expert', 'cuts'), may hold values from -0.125 to 0.125
- dense_out: bfloat16 [8192, 2048], P('cuts', 'expert'), may hold values from -0.0625 to 0.0625
- expert_in: bfloat16 [4, 2048, 8192], P('expert', None, 'cuts'), may hold values from -0.125 to 0.125
- expert_out: bfloat16 [4, 8192, 2048], P('expert', 'cuts'), may hold values from -0.0625 to 0.0625
Outputs:
- layer_out: bfloat16 [4096, 2048], P(('groups', 'expert'), 'cuts'), parts along dimension 0
The draws below stay inside these ranges and needn't reach their ends.
There are 2 independent parts, one for each index of `groups`. The reference program is written for one: setup_inputs(seed, part) draws one part's arguments, and reference() takes and returns one part's arrays. A program takes and returns all parts, laid end to end along the dimension named above; an argument that names none is the same for every part. Nothing has to cross between parts.
Inputs may be any that keep to these rules, and one draw needn't show every extreme that they name: `route`: within the rows of one device (aligned blocks of 512 rows) no expert is named by more than 192 rows; in some blocks one expert is named by exactly 192 rows.
All inputs are finite; a program needn't handle non-finite values.
Results may differ from the reference program's by a relative error of at most 0.0095.
Values may be sent and summed in bfloat16 or wider, within the bound.
A program may use at most 128 MiB of HBM per device.

```python
import math
import jax
import jax.numpy as jnp
import numpy as np
from jax import lax

D = 2048
FF = 8192
TOK_E = 512
EXPERTS = 4
CAP = 192
TOKENS = 2048
N_EXPERT = 4
N_CUTS = 4


def levels(stream_key, dims, shards, least, top_value):
    def one(dim, shards_of):
        draws = jax.random.uniform(jax.random.fold_in(jax.random.fold_in(stream_key, 6), dim), (shards_of,), jnp.float32, least / len(shards), top_value / len(shards))
        return jnp.repeat(jnp.exp(draws), dims[dim] // shards_of).reshape((-1,) + (1,) * (len(dims) - dim - 1))

    factor_of = one(*shards[0])
    for cut in shards[1:]:
        factor_of = factor_of * one(*cut)
    return factor_of


def shared_out(stream_key, own, number, rows, amount, top, limit, skew):
    sequence = jax.random.permutation(stream_key, amount)
    crowded, usual = portions_of(amount, rows * top, limit, skew, True), portions_of(amount, rows * top, limit, skew, False)
    places = jnp.arange(amount)

    def named(tallies, rotation):
        used = int((tallies > 0).sum())
        fixed = max(1, used // 4)
        shifted = fixed + (places - fixed + rotation * (used - fixed)) % max(1, amount - fixed)
        return jnp.zeros((amount,), jnp.int32).at[sequence[jnp.where(places < fixed, places, shifted)]].set(jnp.asarray(tallies, jnp.int32))

    tallies = jnp.where(number % 4 == 0, named(crowded, number // 4), named(usual, number - number // 4 - 1))
    mixed = jax.random.permutation(jax.random.fold_in(own, 3), amount)
    donor, sink = mixed[0:amount // 2 * 2:2], mixed[1:amount // 2 * 2:2]
    margin = jnp.minimum(tallies[donor] - 1, limit - tallies[sink]) // 2
    margin = jnp.where((donor == sequence[0]) | (sink == sequence[0]) | (tallies[sink] == 0), 0, jnp.maximum(margin, 0))
    shifted = jax.random.randint(jax.random.fold_in(own, 4), (amount // 2,), 0, 1 << 20) % (margin + 1)
    tallies = tallies.at[donor].add(-shifted).at[sink].add(shifted)
    items = jnp.searchsorted(jnp.cumsum(tallies), jnp.arange(rows * top), side="right").astype(jnp.int32)
    listing = items.reshape(top, rows).T
    listing = listing[jax.random.permutation(jax.random.fold_in(own, 1), rows)]
    rotation = jax.random.randint(jax.random.fold_in(own, 2), (rows, 1), 0, top)
    return jnp.take_along_axis(listing, (jnp.arange(top)[None, :] + rotation) % top, axis=1)


def portions_of(number_of, total, reach, skew, full):
    weights = [(1 << 20) // math.isqrt(rank ** skew) + 1 for rank in range(1, number_of + 1)]
    largest = reach if full else min(reach, max(-(-total // number_of), total * weights[0] // sum(weights)))
    least = 1 if total - largest >= number_of - 1 else 0
    counts, surplus = [largest] + [least] * (number_of - 1), total - largest - least * (number_of - 1)
    while surplus > 0:
        free = [i for i in range(1, number_of) if counts[i] < largest] or [i for i in range(1, number_of) if counts[i] < reach]
        mass, left = sum([weights[i] for i in free]), surplus
        for i in free:
            more = min(reach - counts[i], max(1, left * weights[i] // mass), surplus)
            counts[i] = counts[i] + more
            surplus = surplus - more
    return np.array(counts)


def normal_values(rng, dims, deviation, bound, shards=(), kind=jnp.bfloat16):
    drawn = deviation * jax.random.normal(rng, dims, jnp.float32)
    if shards:
        drawn = drawn * levels(rng, dims, shards, -0.22, 0.18)
    return jnp.clip(drawn, -bound, bound).astype(kind)


def setup_inputs(seed: int = 0, part: int = 0) -> dict:
    arg_keys = jax.random.split(jax.random.key(seed), 9)
    part_keys = jax.random.split(jax.random.fold_in(arg_keys[8], part), 9)
    tokens = normal_values(part_keys[0], (TOKENS, D), 1.0, 6.0, ((0, 4),))
    route_keys = jax.random.split(jax.random.fold_in(part_keys[1], 1), TOKENS // TOK_E)
    route_turns = jax.random.permutation(jax.random.fold_in(part_keys[1], 3), TOKENS // TOK_E)
    route = jax.vmap(lambda own, number: shared_out(jax.random.fold_in(part_keys[1], 2), own, number, TOK_E, EXPERTS, 1, CAP, 2))(route_keys, route_turns).reshape((TOKENS, 1))
    gate_prob = jnp.clip(jnp.exp(math.log(1.0) - 1.609438 * jax.random.uniform(part_keys[2], (TOKENS,), jnp.float32) ** levels(part_keys[2], (TOKENS,), ((0, 4),), -0.2, 0.2)), 0.2, 1.0)
    norm_gain = jnp.clip(1.0 + 0.1 * jax.random.normal(arg_keys[3], (D,), jnp.float32), 0.5, 1.5)
    dense_in = normal_values(arg_keys[4], (D, FF), D ** -0.5, 0.125, ((0, 4), (1, 4)))
    dense_out = normal_values(arg_keys[5], (FF, D), FF ** -0.5, 0.0625, ((0, 4), (1, 4)))
    expert_in = normal_values(arg_keys[6], (EXPERTS, D, FF), D ** -0.5, 0.125, ((0, 4), (2, 4)))
    expert_out = normal_values(arg_keys[7], (EXPERTS, FF, D), FF ** -0.5, 0.0625, ((0, 4), (1, 4)))
    return {"tokens": tokens, "route": route, "gate_prob": gate_prob, "norm_gain": norm_gain, "dense_in": dense_in, "dense_out": dense_out, "expert_in": expert_in, "expert_out": expert_out}


def normalize(tokens, norm_gain):
    widened = tokens.astype(jnp.float32)
    meansq = lax.optimization_barrier(jnp.mean(widened * widened, axis=-1, keepdims=True))
    return (widened * lax.rsqrt(meansq + 1e-06) * norm_gain).astype(jnp.bfloat16)

def sliced_product(act, weight):
    rows = act.shape[0]
    width = FF // N_CUTS
    act_parts = act.reshape(rows, N_CUTS, width).transpose(1, 0, 2)
    weight_parts = weight.reshape(N_CUTS, width, D)

    def add_slice(total, operands):
        act_part, weight_part = operands
        partial_out = jnp.dot(act_part, weight_part, preferred_element_type=jnp.float32)
        rounded = lax.optimization_barrier(partial_out.astype(jnp.bfloat16)).astype(jnp.float32)
        return (total + rounded, None)
    total, unused = lax.scan(add_slice, jnp.zeros((rows, D), jnp.float32), (act_parts, weight_parts))
    return total

def run_expert(operands):
    gathered, weight_in, weight_out = operands
    inner = jax.nn.gelu(jnp.dot(gathered, weight_in, preferred_element_type=jnp.float32)).astype(jnp.bfloat16)
    return sliced_product(inner, weight_out).astype(jnp.bfloat16)

def reference(tokens, route, gate_prob, norm_gain, dense_in, dense_out, expert_in, expert_out):
    normed = normalize(tokens, norm_gain)
    dense_act = jax.nn.gelu(jnp.dot(normed, dense_in, preferred_element_type=jnp.float32)).astype(jnp.bfloat16)
    dense = sliced_product(dense_act, dense_out)
    picked = route[:, 0].reshape(N_EXPERT, TOK_E)
    labels = jnp.arange(EXPERTS, dtype=jnp.int32)
    one_hot = (picked[:, :, None] == labels[None, None, :]).astype(jnp.int32)
    before = jnp.cumsum(one_hot, axis=1) - one_hot
    position = lax.optimization_barrier(jnp.sum(before * one_hot, axis=-1))
    block_ids = jnp.arange(N_EXPERT, dtype=jnp.int32)[:, None]
    target = (picked * (N_EXPERT * CAP) + block_ids * CAP + position).reshape(-1).astype(jnp.int32)
    buffer = jnp.zeros((EXPERTS * N_EXPERT * CAP, D), jnp.bfloat16).at[target].set(normed)
    buffer = buffer.reshape(EXPERTS, N_EXPERT * CAP, D)
    results = lax.map(run_expert, (buffer, expert_in, expert_out)).reshape(-1, D)
    expert_res = results[target].astype(jnp.float32)
    layer_out = tokens.astype(jnp.float32) + dense + gate_prob[:, None] * expert_res
    return layer_out.astype(jnp.bfloat16)
```

```python
import functools

import jax
import jax.numpy as jnp
from jax import lax
from jax.experimental import pallas as pl
from jax.experimental.pallas import tpu as pltpu
from jax.sharding import PartitionSpec as P

SUBS = (4, 4)
EARLY = 1


def kernel(G, E, Z, cap, nk, tokens, route, gate, gain, din, dout, ein_h, eout_h, out,
           win, wout, ein, eout, tok, normed, disp, dispq, arrived, hbuf, pown, psend, po, rpo, pd, rpd,
           ret, rret, base, pk,
           loc, own_s, own_r, d1_s, d1_r, dx_s, dx_r, ag_s, ag_r, pq_s, pq_r,
           wx_s, wx_r, wy_s, wy_r, wp_s, wp_r, zo_s, zo_r, zd_s, zd_r, ret_s, ret_r):
    f32, bf16 = jnp.float32, jnp.bfloat16
    T, D = tok.shape
    F = ein.shape[1]
    De = D // E
    share = D // Z
    C = E // 2
    wide = share // nk
    tn = min(256, wide)
    units = range(2, E)
    g, e, z = lax.axis_index("groups"), lax.axis_index("expert"), lax.axis_index("cuts")
    chip, core = e // 2, lax.rem(e, 2)
    partner = chip * 2 + 1 - core
    above, below = lax.rem(z + 1, Z), lax.rem(z + Z - 1, Z)
    upper = (2 * z) // Z

    def remote(src, dst, send, recv, gg=None, ee=None, zz=None):
        return pltpu.make_async_remote_copy(
            src_ref=src, dst_ref=dst, send_sem=send, recv_sem=recv,
            device_id={
                "groups": g if gg is None else gg,
                "expert": e if ee is None else ee,
                "cuts": z if zz is None else zz,
            },
            device_id_type=pl.DeviceIdType.MESH,
        )

    def when(condition):
        return pl.when(condition)

    def expert_at(kc, j):
        other = lax.rem(chip + kc + C, C)
        return other * 2 + (core if j == 0 else 1 - core)

    my_rows = pl.ds(pl.multiple_of(e * De, De), De)
    locals_ = [
        pltpu.make_async_copy(tokens, tok, loc.at[0]),
        pltpu.make_async_copy(ein_h.at[0], ein, loc.at[1]),
        pltpu.make_async_copy(eout_h.at[0], eout, loc.at[2]),
        pltpu.make_async_copy(din, win.at[my_rows, :], loc.at[3]),
        pltpu.make_async_copy(dout, wout.at[:, my_rows], loc.at[4]),
    ]
    locals_[0].start()

    barrier = pltpu.get_barrier_semaphore()
    for k in range(1, E):
        pl.semaphore_signal(barrier, inc=1, device_id={"groups": g, "expert": lax.rem(e + k, E), "cuts": z},
                            device_id_type=pl.DeviceIdType.MESH)
    for k in range(1, Z):
        pl.semaphore_signal(barrier, inc=1, device_id={"groups": g, "expert": e, "cuts": lax.rem(z + k, Z)},
                            device_id_type=pl.DeviceIdType.MESH)
    for k in range(1, G):
        pl.semaphore_signal(barrier, inc=1, device_id={"groups": lax.rem(g + k, G), "expert": e, "cuts": z},
                            device_id_type=pl.DeviceIdType.MESH)
    pl.semaphore_wait(barrier, (E - 1) + (Z - 1) + (G - 1))

    own_copies = [
        remote(din, win.at[my_rows, :], own_s.at[0], own_r.at[0], ee=partner),
        remote(dout, wout.at[:, my_rows], own_s.at[1], own_r.at[1], ee=partner),
    ]

    def block(m, p, s):
        if m == 0:
            n = De // G // SUBS[0]
            return p * (De // G) + s * n, n, 0, F
        per = SUBS[1] // nk
        n = F // G // per
        return p * (F // G) + (s % per) * n, n, (s // per) * (De // nk), De // nk

    def weight(m, owner, p, s):
        row, n, col, width = block(m, p, s)
        if m == 0:
            return win.at[pl.ds(pl.multiple_of(owner * De + row, n), n), :]
        return wout.at[pl.ds(pl.multiple_of(row, n), n),
                       pl.ds(pl.multiple_of(owner * De + col, width), width)]

    def weight_source(m, p, s):
        row, n, col, width = block(m, p, s)
        return (din, dout)[m].at[pl.ds(pl.multiple_of(row, n), n), pl.ds(col, width)]

    def x_copy(m, kc, s):
        return remote(weight_source(m, g, s), weight(m, e, g, s), wx_s.at[m, kc, s], wx_r.at[m, kc, s],
                      ee=expert_at(kc, 0))

    def y_copy(m, kc, s, dg):
        w = weight(m, expert_at(-kc, 0), g, s)
        return remote(w, w, wy_s.at[m, kc, s, dg], wy_r.at[m, kc, s, dg], gg=lax.rem(g + dg, G))

    def p_copy(m, kc, s, dg):
        w = weight(m, expert_at(-kc, 0), lax.rem(g - dg + G, G), s)
        return remote(w, w, wp_s.at[m, kc, s, dg], wp_r.at[m, kc, s, dg], ee=partner)

    steps = [(m, s) for m in range(2) for s in range(SUBS[m])]
    issued, taken, relayed = [0], [0], [0]

    def issue(upto):
        while issued[0] < min(upto, len(steps)):
            m, s = steps[issued[0]]
            for kc in range(1, C):
                x_copy(m, kc, s).start()
            issued[0] += 1

    def relay(upto):
        while relayed[0] < min(upto, taken[0]):
            m, s = steps[relayed[0]]
            for kc in range(1, C):
                for dg in range(1, G):
                    y_copy(m, kc, s, dg).wait_recv()
                    p_copy(m, kc, s, dg).start()
            relayed[0] += 1

    def take(upto):
        while taken[0] < min(upto, len(steps)):
            m, s = steps[taken[0]]
            for kc in range(1, C):
                x_copy(m, kc, s).wait_recv()
                for dg in range(1, G):
                    y_copy(m, kc, s, dg).start()
                p_copy(m, kc, s, 0).start()
            taken[0] += 1

    def collect(m, subs):
        for s in subs:
            for kc in range(1, C):
                for dg in range(G):
                    p_copy(m, kc, s, dg).wait_recv()

    issue(EARLY)
    locals_[0].wait()
    for copy in locals_[1:]:
        copy.start()

    nrow = min(64, T)

    def norm_step(i, carry):
        rows = pl.ds(pl.multiple_of(i * nrow, nrow), nrow)
        x = tok[rows, :].astype(f32)
        ms = jnp.mean(x * x, axis=-1, keepdims=True)
        normed[rows, :] = (x * lax.rsqrt(ms + 1e-06) * gain[...]).astype(bf16)
        return carry

    lax.fori_loop(0, T // nrow, norm_step, 0)

    picked = route[...]
    one_hot = (lax.broadcasted_iota(jnp.int32, (T, 128), 1) == picked).astype(f32)
    lower = (lax.broadcasted_iota(jnp.int32, (T, T), 1) < lax.broadcasted_iota(jnp.int32, (T, T), 0))
    before = jnp.dot(lower.astype(f32).astype(bf16), one_hot.astype(bf16), preferred_element_type=f32)
    position = jnp.sum(before * one_hot, axis=1, keepdims=True)
    slot_col = picked.astype(f32) * float(cap) + position
    slot_row = jnp.transpose(jnp.broadcast_to(slot_col, (T, 128)))[0:1, :]

    def slice_at(s):
        return pl.ds(pl.multiple_of(s * share, share), share)

    def picks(q):
        dest = expert_at(q // 2, q % 2)
        wanted = slot_row - (dest * cap).astype(f32)
        return (lax.broadcasted_iota(jnp.int32, (cap, T), 0).astype(f32) == wanted).astype(f32).astype(bf16)

    def fill_slice(q, x, s):
        disp[x, (q - 2) * cap:(q - 1) * cap, :] = jnp.dot(
            picks(q), normed[:, slice_at(s)], preferred_element_type=f32).astype(bf16)

    def fill(q, dst):
        pick = picks(q)
        dn = min(512, D)

        def step(i, carry):
            cols = pl.ds(pl.multiple_of(i * dn, dn), dn)
            dst[0:cap, cols] = jnp.dot(pick, normed[:, cols], preferred_element_type=f32).astype(bf16)
            return carry

        lax.fori_loop(0, D // dn, step, 0)

    ends = ((0, Z - 1), (Z - 1, 0))

    def dx_copy(q, x, s):
        return remote(disp.at[x, pl.ds((q - 2) * cap, cap), :], arrived.at[pl.ds(q * cap, cap), slice_at(s)],
                      dx_s.at[q, x], dx_r.at[q, x], ee=expert_at(q // 2, q % 2))

    d1_copy = remote(dispq, arrived.at[pl.ds(cap, cap), :], d1_s.at[0], d1_r.at[0], ee=partner)

    pending = None
    for q in units:
        fill_slice(q, 0, z)
        if pending is not None:
            dx_copy(pending, 0, z).start()
        pending = q
    for at, s in ends:
        @when(z == at)
        def _():
            for q in units:
                fill_slice(q, 1, s)
    if pending is not None:
        dx_copy(pending, 0, z).start()
    fill(1, dispq)
    for at, s in ends:
        @when(z == at)
        def _():
            for q in units:
                dx_copy(q, 1, s).start()
    issue(len(steps))
    fill(0, arrived)
    d1_copy.start()
    for copy in own_copies:
        copy.start()

    def hop(q, way, t, s):
        part = arrived.at[pl.ds(q * cap, cap), slice_at(s)]
        return remote(part, part, ag_s.at[q, way, t], ag_r.at[q, way, t], zz=below if way else above)

    def gather(q, t):
        if t == 0:
            dx_copy(q, 0, z).wait_recv()

        @when(z >= t)
        def _():
            if t > 0:
                hop(q, 0, t, z - t).wait_recv()
        if t < Z - 2:
            @when((z >= t) & (z < Z - 1))
            def _():
                hop(q, 0, t + 1, z - t).start()

        @when(z + t <= Z - 1)
        def _():
            if t > 0:
                hop(q, 1, t, z + t).wait_recv()
        if t < Z - 2:
            @when((z + t <= Z - 1) & (z > 0))
            def _():
                hop(q, 1, t + 1, z + t).start()

    def hidden(load, rows, w, lo=0, hi=None):
        def step(i, carry):
            cols = pl.ds(pl.multiple_of(i * 256, 256), 256)
            acc = jnp.dot(load(), w[:, cols], preferred_element_type=f32)
            hbuf[0:rows, cols] = jax.nn.gelu(acc).astype(bf16)
            return carry

        lax.fori_loop(lo, F // 256 if hi is None else hi, step, 0)

    blocks = F // 256

    def part_of(i, n):
        return i * blocks // n, (i + 1) * blocks // n

    pair = 2 * cap
    take(EARLY)
    col = lax.broadcasted_iota(jnp.int32, (T, pair), 1).astype(f32)
    here = slot_col - (e * cap).astype(f32)
    there = slot_col - (partner * cap).astype(f32) + float(cap)
    pk[...] = (((col == here) & (col < cap)) | ((col == there) & (col >= cap))).astype(f32).astype(bf16)

    locals_[1].wait()
    d1_copy.wait_recv()
    for i in range(4):
        hidden(lambda: arrived[0:pair, :], pair, ein, *part_of(i, 4))
        if i == 1:
            for q in units:
                gather(q, 0)

    locals_[2].wait()

    def own_step(i, carry):
        cols = pl.ds(pl.multiple_of(i * 256, 256), 256)
        acc = jnp.dot(hbuf[0:pair, :], eout[:, cols], preferred_element_type=f32).astype(bf16)
        pown[0:cap, cols] = acc[0:cap, :]
        psend[:, cols] = acc[cap:pair, :]
        return carry

    own_blocks = D // 256
    lax.fori_loop(0, own_blocks // 2, own_step, 0)
    if Z > 2:
        for q in units:
            gather(q, 1)
    relay(EARLY)
    lax.fori_loop(own_blocks // 2, own_blocks, own_step, 0)

    @when(z == 0)
    def _():
        rpo[0] = jnp.zeros(rpo.shape[1:], bf16)
        rpd[0] = jnp.zeros(rpd.shape[1:], bf16)

    @when(z == Z - 1)
    def _():
        rpo[Z] = jnp.zeros(rpo.shape[1:], bf16)
        rpd[Z] = jnp.zeros(rpd.shape[1:], bf16)

    pq_copy = remote(psend, pown.at[pl.ds(cap, cap), :], pq_s.at[0], pq_r.at[0], ee=partner)
    pq_copy.start()

    def zo_copy(q, d, slot, to):
        rows = pl.ds((q - 2) * cap, cap)
        return remote(po.at[d, rows, :], rpo.at[slot, rows, :], zo_s.at[q, d], zo_r.at[q, slot], zz=to)

    def back_slot(d, to):
        return Z if d == to else d

    def zo_edge(q, i):
        @when(z == 0)
        def _():
            zo_copy(q, Z - 1 - i, Z - 1 - i, 1).start()

        @when(z == Z - 1)
        def _():
            zo_copy(q, i, back_slot(i, Z - 2), Z - 2).start()

    def expert_unit(q):
        for t in range(2, Z - 1):
            gather(q, t)
        for at, s in ends:
            @when(z == at)
            def _():
                dx_copy(q, 1, s).wait_recv()
        hidden(lambda: arrived[q * cap:(q + 1) * cap, :], cap, ein)
        rows = slice((q - 2) * cap, (q - 1) * cap)
        for i in range(Z):
            d = (1 - upper) * (Z - 1 - i) + upper * i

            def step(k, carry):
                acc = jnp.dot(hbuf[0:cap, :], eout[:, pl.ds(pl.multiple_of(d * share + k * 256, 256), 256)],
                              preferred_element_type=f32)
                po[d, rows, pl.ds(pl.multiple_of(k * 256, 256), 256)] = acc.astype(bf16)
                return carry

            lax.fori_loop(0, share // 256, step, 0)
            if i > 0:
                zo_edge(q, i - 1)

    def zo_up(q, d):
        @when((z > 0) & (z < d))
        def _():
            rows = slice((q - 2) * cap, (q - 1) * cap)
            zo_copy(q, d, d, above).wait_recv()
            po[d, rows, :] = (po[d, rows, :].astype(f32) + rpo[d, rows, :].astype(f32)).astype(bf16)
            zo_copy(q, d, d, above).start()

    def zo_down(q, d):
        @when((z < Z - 1) & (z > d))
        def _():
            rows = slice((q - 2) * cap, (q - 1) * cap)
            zo_copy(q, d, d, below).wait_recv()
            po[d, rows, :] = (po[d, rows, :].astype(f32) + rpo[d, rows, :].astype(f32)).astype(bf16)

        for slot, near in ((d, z > d + 1), (Z, z == d + 1)):
            @when((z < Z - 1) & near)
            def _():
                zo_copy(q, d, slot, below).start()

    def zo_pass(q, t):
        @when(upper == 0)
        def _():
            zo_up(q, Z - 1 - t)
            zo_down(q, t)

        @when(upper == 1)
        def _():
            zo_down(q, t)
            zo_up(q, Z - 1 - t)

    def ret_copy(q):
        rows = pl.ds((q - 2) * cap, cap)
        return remote(ret.at[rows, :], rret.at[rows, :], ret_s.at[q], ret_r.at[q], ee=expert_at(-(q // 2), q % 2))

    def zo_final(q):
        @when(z > 0)
        def _():
            zo_copy(q, z, z, above).wait_recv()

        @when(z < Z - 1)
        def _():
            zo_copy(q, z, Z, above).wait_recv()
        rows = slice((q - 2) * cap, (q - 1) * cap)
        ret[rows, :] = (po[z, rows, :].astype(f32) + rpo[z, rows, :].astype(f32)
                        + rpo[Z, rows, :].astype(f32)).astype(bf16)

    for q in units:
        expert_unit(q)
        take(EARLY + 1)

    first = SUBS[0]
    half = [q for q in units][:max(1, len(units) // 2)] if len(units) else []
    rest = [q for q in units][len(half):]
    for t in range(Z - 1):
        for q in half:
            zo_pass(q, t)
        take(EARLY + 2 + t)
        relay(EARLY + 1 + t)
    for q in half:
        zo_final(q)
    take(first)
    relay(first)
    locals_[3].wait()
    own_copies[0].wait_recv()
    collect(0, range(SUBS[0]))
    for q in half:
        ret_copy(q).start()
    for i in range(4):
        hidden(lambda: normed[...], T, win, *part_of(i, 4))
        if i < Z - 1:
            for q in rest:
                zo_pass(q, i)
        if i in (0, 2):
            take(first + 1 + i // 2)
    for t in range(4, Z - 1):
        for q in rest:
            zo_pass(q, t)

    def zd_copy(d, slot, c, to):
        cols = pl.ds(c * wide, wide)
        return remote(pd.at[d, :, cols], rpd.at[slot, :, cols], zd_s.at[d, c], zd_r.at[slot, c], zz=to)

    locals_[4].wait()
    own_copies[1].wait_recv()
    pq_copy.wait_recv()
    mine = Z // C if Z % C == 0 else 0

    def slice_number(i):
        if C == 2 and Z % 2 == 0:
            low = i if i < mine else Z - 1 - (i - mine)
            return chip * (Z - 1 - low) + (1 - chip) * low
        return lax.rem(chip * mine + i, Z)

    def dense(i, c):
        d = slice_number(i)

        def step(k, carry):
            cols = pl.ds(pl.multiple_of(d * share + c * wide + k * tn, tn), tn)
            acc = jnp.dot(hbuf[0:T, :], wout[:, cols], preferred_element_type=f32)
            res = jnp.dot(pk[...], pown[:, cols], preferred_element_type=f32)
            pd[d, :, pl.ds(pl.multiple_of(c * wide + k * tn, tn), tn)] = (acc + gate[...] * res).astype(bf16)
            return carry

        lax.fori_loop(0, wide // tn, step, 0)

        @when((z == 0) & (d > 0))
        def _():
            zd_copy(d, d, c, above).start()

        for slot, near in ((d, z > d + 1), (Z, z == d + 1)):
            @when((z == Z - 1) & near)
            def _():
                zd_copy(d, slot, c, below).start()

    def zd_pass(i, c):
        d = slice_number(i)
        cols = pl.ds(c * wide, wide)

        @when((z > 0) & (z < Z - 1) & (z != d))
        def _():
            zd_copy(d, d, c, above).wait_recv()
            pd[d, :, cols] = (pd[d, :, cols].astype(f32) + rpd[d, :, cols].astype(f32)).astype(bf16)

        @when((z > 0) & (z < d))
        def _():
            zd_copy(d, d, c, above).start()

        for slot, near in ((d, z > d + 1), (Z, z == d + 1)):
            @when((z < Z - 1) & near)
            def _():
                zd_copy(d, slot, c, below).start()

    trow = min(128, T)
    residual = slice_at(z)

    def combine_experts():
        for q in units:
            ret_copy(q).wait_recv()
        for i in range(T // trow):
            rows = slice(i * trow, (i + 1) * trow)
            res = jnp.zeros((trow, share), f32)
            for q in units:
                wanted = slot_col[rows, :] - (expert_at(q // 2, q % 2) * cap).astype(f32)
                pick = (lax.broadcasted_iota(jnp.int32, (trow, cap), 1).astype(f32) == wanted)
                res = res + jnp.dot(pick.astype(f32).astype(bf16), rret[(q - 2) * cap:(q - 1) * cap, :],
                                    preferred_element_type=f32)
            base[rows, :] = tok[rows, residual].astype(f32) + gate[rows, :] * res

    def finish(c):
        cols = slice(c * wide, (c + 1) * wide)

        @when(z > 0)
        def _():
            zd_copy(z, z, c, above).wait_recv()

        @when(z < Z - 1)
        def _():
            zd_copy(z, Z, c, above).wait_recv()

        for i in range(T // trow):
            rows = slice(i * trow, (i + 1) * trow)
            total = pd[z, rows, cols].astype(f32) + rpd[z, rows, cols].astype(f32) + rpd[Z, rows, cols].astype(f32)
            out[rows, cols] = (base[rows, cols] + total).astype(bf16)

    per = SUBS[1] // nk
    for i in range(mine):
        for c in range(nk):
            dense(i, c)
    for q in rest:
        zo_final(q)
    for c in range(nk):
        last = first + (c + 1) * per
        take(last)
        if c == 0:
            for q in rest:
                ret_copy(q).start()
        relay(last)
        collect(1, range(c * per, (c + 1) * per))
        for i in range(mine, Z):
            dense(i, c)
        if c == 0:
            for i in range(mine):
                for k in range(nk):
                    zd_pass(i, k)
    combine_experts()
    for c in range(nk):
        for i in range(mine, Z):
            zd_pass(i, c)
        finish(c)

    for copy in own_copies:
        copy.wait_send()
    d1_copy.wait_send()
    pq_copy.wait_send()
    for q in units:
        dx_copy(q, 0, z).wait_send()
        ret_copy(q).wait_send()
        for at, s in ends:
            @when(z == at)
            def _():
                dx_copy(q, 1, s).wait_send()
        for t in range(1, Z - 1):
            @when((z >= t - 1) & (z < Z - 1))
            def _():
                hop(q, 0, t, z - t + 1).wait_send()

            @when((z + t - 1 <= Z - 1) & (z > 0))
            def _():
                hop(q, 1, t, z + t - 1).wait_send()
    for m in range(2):
        for s in range(SUBS[m]):
            for kc in range(1, C):
                x_copy(m, kc, s).wait_send()
                for dg in range(1, G):
                    y_copy(m, kc, s, dg).wait_send()
                for dg in range(G):
                    p_copy(m, kc, s, dg).wait_send()
    for d in range(Z):
        @when(z != d)
        def _():
            for q in units:
                zo_copy(q, d, d, above).wait_send()
            for c in range(nk):
                zd_copy(d, d, c, above).wait_send()


def local(tokens, route, gate_prob, norm_gain, dense_in, dense_out, expert_in, expert_out):
    G, E, Z = lax.axis_size("groups"), lax.axis_size("expert"), lax.axis_size("cuts")
    T, D = tokens.shape
    F = dense_in.shape[1]
    share = D // Z
    De = D // E
    cap = max(2, 3 * T // (2 * E))
    C = E // 2
    others = (E - 2) * cap
    nk = 2 if De == share and share % 256 == 0 else 1
    bf16 = jnp.bfloat16
    any_, vmem = pl.BlockSpec(memory_space=pl.ANY), pl.BlockSpec(memory_space=pltpu.VMEM)
    dma = pltpu.SemaphoreType.DMA
    subs = max(SUBS)
    return pl.pallas_call(
        functools.partial(kernel, G, E, Z, cap, nk),
        out_shape=jax.ShapeDtypeStruct((T, share), bf16),
        in_specs=[any_, vmem, vmem, vmem, any_, any_, any_, any_],
        out_specs=vmem,
        scratch_shapes=[
            pltpu.VMEM((D, F), bf16), pltpu.VMEM((F, D), bf16),
            pltpu.VMEM((D, F), bf16), pltpu.VMEM((F, D), bf16),
            pltpu.VMEM((T, D), bf16), pltpu.VMEM((T, D), bf16),
            pltpu.VMEM((2, others, share), bf16), pltpu.VMEM((cap, D), bf16), pltpu.VMEM((E * cap, D), bf16),
            pltpu.VMEM((max(T, 2 * cap), F), bf16),
            pltpu.VMEM((2 * cap, D), bf16), pltpu.VMEM((cap, D), bf16),
            pltpu.VMEM((Z, others, share), bf16), pltpu.VMEM((Z + 1, others, share), bf16),
            pltpu.VMEM((Z, T, share), bf16), pltpu.VMEM((Z + 1, T, share), bf16),
            pltpu.VMEM((others, share), bf16), pltpu.VMEM((others, share), bf16),
            pltpu.VMEM((T, share), jnp.float32), pltpu.VMEM((T, 2 * cap), bf16),
            dma((5,)), dma((2,)), dma((2,)), dma((1,)), dma((1,)), dma((E, 2)), dma((E, 2)),
            dma((E, 2, Z)), dma((E, 2, Z)), dma((1,)), dma((1,)),
            dma((2, C, subs)), dma((2, C, subs)),
            dma((2, C, subs, G)), dma((2, C, subs, G)), dma((2, C, subs, G)), dma((2, C, subs, G)),
            dma((E, Z)), dma((E, Z + 1)), dma((Z, nk)), dma((Z + 1, nk)), dma((E,)), dma((E,)),
        ],
        compiler_params=pltpu.CompilerParams(
            collective_id=0, has_side_effects=True, vmem_limit_bytes=67043328
        ),
    )(tokens, route, gate_prob[:, None], norm_gain[None, :], dense_in, dense_out, expert_in, expert_out)


def solution(mesh):
    return jax.shard_map(
        local,
        mesh=mesh,
        in_specs=(
            P(("groups", "expert"), None),
            P(("groups", "expert"), None),
            P(("groups", "expert")),
            P(),
            P("expert", "cuts"),
            P("cuts", "expert"),
            P("expert", None, "cuts"),
            P("expert", "cuts", None),
        ),
        out_specs=P(("groups", "expert"), "cuts"),
        check_vma=False,
    )
```

```python
import functools

import jax
import jax.numpy as jnp
from jax import lax
from jax.experimental import pallas as pl
from jax.experimental.pallas import tpu as pltpu
from jax.sharding import PartitionSpec as P

EARLY = 1


def kernel(G, E, Z, cap, nk, SUBS, tokens, route, gate, gain, din, dout, ein_h, eout_h, out,
           win, wout, ein, eout, tok, normed, disp, dispq, arrived, hbuf, pown, psend, po, rpo, pd, rpd,
           ret, rret, base, pk, turned,
           loc, own_s, own_r, d1_s, d1_r, dx_s, dx_r, ag_s, ag_r, pq_s, pq_r,
           wx_s, wx_r, wy_s, wy_r, wp_s, wp_r, zo_s, zo_r, zd_s, zd_r, ret_s, ret_r):
    f32, bf16 = jnp.float32, jnp.bfloat16
    T, D = tok.shape
    F = ein.shape[1]
    De = D // E
    share = D // Z
    C = E // 2
    wide = share // nk
    tn = min(256, wide)
    units = range(2, E)
    fast, slow = units[:(E - 2) // 2], units[(E - 2) // 2:]
    g, e, z = lax.axis_index("groups"), lax.axis_index("expert"), lax.axis_index("cuts")
    chip, core = e // 2, lax.rem(e, 2)
    partner = chip * 2 + 1 - core
    above, below = lax.rem(z + 1, Z), lax.rem(z + Z - 1, Z)
    upper = (2 * z) // Z

    def remote(src, dst, send, recv, gg=None, ee=None, zz=None):
        return pltpu.make_async_remote_copy(
            src_ref=src, dst_ref=dst, send_sem=send, recv_sem=recv,
            device_id={
                "groups": g if gg is None else gg,
                "expert": e if ee is None else ee,
                "cuts": z if zz is None else zz,
            },
            device_id_type=pl.DeviceIdType.MESH,
        )

    def when(condition):
        return pl.when(condition)

    def expert_at(kc, j):
        other = lax.rem(chip + kc + C, C)
        return other * 2 + (core if j == 0 else 1 - core)

    my_rows = pl.ds(pl.multiple_of(e * De, De), De)
    locals_ = [
        pltpu.make_async_copy(tokens, tok, loc.at[0]),
        pltpu.make_async_copy(ein_h.at[0], ein, loc.at[1]),
        pltpu.make_async_copy(eout_h.at[0], eout, loc.at[2]),
        pltpu.make_async_copy(din, win.at[my_rows, :], loc.at[3]),
        pltpu.make_async_copy(dout, wout.at[:, my_rows], loc.at[4]),
    ]
    locals_[0].start()

    barrier = pltpu.get_barrier_semaphore()
    for k in range(1, E):
        pl.semaphore_signal(barrier, inc=1, device_id={"groups": g, "expert": lax.rem(e + k, E), "cuts": z},
                            device_id_type=pl.DeviceIdType.MESH)
    for k in range(1, Z):
        pl.semaphore_signal(barrier, inc=1, device_id={"groups": g, "expert": e, "cuts": lax.rem(z + k, Z)},
                            device_id_type=pl.DeviceIdType.MESH)
    for k in range(1, G):
        pl.semaphore_signal(barrier, inc=1, device_id={"groups": lax.rem(g + k, G), "expert": e, "cuts": z},
                            device_id_type=pl.DeviceIdType.MESH)
    pl.semaphore_wait(barrier, (E - 1) + (Z - 1) + (G - 1))

    own_copies = [
        remote(din, win.at[my_rows, :], own_s.at[0], own_r.at[0], ee=partner),
        remote(dout, wout.at[:, my_rows], own_s.at[1], own_r.at[1], ee=partner),
    ]

    def block(m, p, s):
        if m == 0:
            n = De // G // SUBS[0]
            return p * (De // G) + s * n, n, 0, F
        per = SUBS[1] // nk
        n = F // G // per
        return p * (F // G) + (s % per) * n, n, (s // per) * (De // nk), De // nk

    def weight(m, owner, p, s):
        row, n, col, width = block(m, p, s)
        if m == 0:
            return win.at[pl.ds(pl.multiple_of(owner * De + row, n), n), :]
        return wout.at[pl.ds(pl.multiple_of(row, n), n),
                       pl.ds(pl.multiple_of(owner * De + col, width), width)]

    def weight_source(m, p, s):
        row, n, col, width = block(m, p, s)
        return (din, dout)[m].at[pl.ds(pl.multiple_of(row, n), n), pl.ds(col, width)]

    def x_copy(m, kc, s):
        return remote(weight_source(m, g, s), weight(m, e, g, s), wx_s.at[m, kc, s], wx_r.at[m, kc, s],
                      ee=expert_at(kc, 0))

    def y_copy(m, kc, s, dg):
        w = weight(m, expert_at(-kc, 0), g, s)
        return remote(w, w, wy_s.at[m, kc, s, dg], wy_r.at[m, kc, s, dg], gg=lax.rem(g + dg, G))

    def p_copy(m, kc, s, dg):
        w = weight(m, expert_at(-kc, 0), lax.rem(g - dg + G, G), s)
        return remote(w, w, wp_s.at[m, kc, s, dg], wp_r.at[m, kc, s, dg], ee=partner)

    steps = [(m, s) for m in range(2) for s in range(SUBS[m])]
    issued, taken, relayed = [0], [0], [0]

    def issue(upto):
        while issued[0] < min(upto, len(steps)):
            m, s = steps[issued[0]]
            for kc in range(1, C):
                x_copy(m, kc, s).start()
            issued[0] += 1

    def relay(upto):
        while relayed[0] < min(upto, taken[0]):
            m, s = steps[relayed[0]]
            for kc in range(1, C):
                for dg in range(1, G):
                    y_copy(m, kc, s, dg).wait_recv()
                    p_copy(m, kc, s, dg).start()
            relayed[0] += 1

    def take(upto):
        while taken[0] < min(upto, len(steps)):
            m, s = steps[taken[0]]
            for kc in range(1, C):
                x_copy(m, kc, s).wait_recv()
                for dg in range(1, G):
                    y_copy(m, kc, s, dg).start()
                p_copy(m, kc, s, 0).start()
            taken[0] += 1

    def collect(m, subs):
        for s in subs:
            for kc in range(1, C):
                for dg in range(G):
                    p_copy(m, kc, s, dg).wait_recv()

    issue(EARLY)
    locals_[0].wait()
    for copy in locals_[1:]:
        copy.start()

    nrow = min(64, T)

    def norm_step(i, carry):
        rows = pl.ds(pl.multiple_of(i * nrow, nrow), nrow)
        x = tok[rows, :].astype(f32)
        ms = jnp.mean(x * x, axis=-1, keepdims=True)
        normed[rows, :] = (x * lax.rsqrt(ms + 1e-06) * gain[...]).astype(bf16)
        return carry

    lax.fori_loop(0, T // nrow, norm_step, 0)

    picked = route[...]
    lanes = -(-E // 8) * 8
    one_hot = (lax.broadcasted_iota(jnp.int32, (lanes, T), 0) == picked).astype(f32)
    earlier = (lax.broadcasted_iota(jnp.int32, (T, T), 0) < lax.broadcasted_iota(jnp.int32, (T, T), 1))
    before = jnp.dot(one_hot.astype(bf16), earlier.astype(f32).astype(bf16), preferred_element_type=f32)
    position = jnp.sum(before * one_hot, axis=0, keepdims=True)
    slot_row = picked.astype(f32) * float(cap) + position

    def slice_at(s):
        return pl.ds(pl.multiple_of(s * share, share), share)

    def picks(q):
        dest = expert_at(q // 2, q % 2)
        wanted = slot_row - (dest * cap).astype(f32)
        return (lax.broadcasted_iota(jnp.int32, (cap, T), 0).astype(f32) == wanted).astype(f32).astype(bf16)

    def fill_slice(q, x, s):
        disp[x, (q - 2) * cap:(q - 1) * cap, :] = jnp.dot(
            picks(q), normed[:, slice_at(s)], preferred_element_type=f32).astype(bf16)

    def fill(q, dst):
        pick = picks(q)
        dn = min(512, D)

        def step(i, carry):
            cols = pl.ds(pl.multiple_of(i * dn, dn), dn)
            dst[0:cap, cols] = jnp.dot(pick, normed[:, cols], preferred_element_type=f32).astype(bf16)
            return carry

        lax.fori_loop(0, D // dn, step, 0)

    ends = ((0, Z - 1), (Z - 1, 0))

    def dx_copy(q, x, s):
        return remote(disp.at[x, pl.ds((q - 2) * cap, cap), :], arrived.at[pl.ds(q * cap, cap), slice_at(s)],
                      dx_s.at[q, x], dx_r.at[q, x], ee=expert_at(q // 2, q % 2))

    d1_copy = remote(dispq, arrived.at[pl.ds(cap, cap), :], d1_s.at[0], d1_r.at[0], ee=partner)

    pending = None
    for q in units:
        fill_slice(q, 0, z)
        if pending is not None:
            dx_copy(pending, 0, z).start()
        pending = q
    for at, s in ends:
        @when(z == at)
        def _():
            for q in fast:
                fill_slice(q, 1, s)
    if pending is not None:
        dx_copy(pending, 0, z).start()
    fill(1, dispq)
    for at, s in ends:
        @when(z == at)
        def _():
            for q in fast:
                dx_copy(q, 1, s).start()
    issue(len(steps))
    fill(0, arrived)
    d1_copy.start()
    for copy in own_copies:
        copy.start()

    def hop(q, way, t, s):
        part = arrived.at[pl.ds(q * cap, cap), slice_at(s)]
        return remote(part, part, ag_s.at[q, way, t], ag_r.at[q, way, t], zz=below if way else above)

    def hops(q):
        return Z - 2 if q in fast else Z - 1

    def gather(q, t):
        if t == 0:
            dx_copy(q, 0, z).wait_recv()

        @when(z >= t)
        def _():
            if t > 0:
                hop(q, 0, t, z - t).wait_recv()
        if t < hops(q):
            @when((z >= t) & (z < Z - 1))
            def _():
                hop(q, 0, t + 1, z - t).start()

        @when(z + t <= Z - 1)
        def _():
            if t > 0:
                hop(q, 1, t, z + t).wait_recv()
        if t < hops(q):
            @when((z + t <= Z - 1) & (z > 0))
            def _():
                hop(q, 1, t + 1, z + t).start()

    def hidden(load, rows, w, lo=0, hi=None):
        def step(i, carry):
            cols = pl.ds(pl.multiple_of(i * 256, 256), 256)
            acc = jnp.dot(load(), w[:, cols], preferred_element_type=f32)
            hbuf[0:rows, cols] = jax.nn.gelu(acc).astype(bf16)
            return carry

        lax.fori_loop(lo, F // 256 if hi is None else hi, step, 0)

    blocks = F // 256

    def part_of(i, n):
        return i * blocks // n, (i + 1) * blocks // n

    pair = 2 * cap
    take(EARLY)
    first_row = lax.broadcasted_iota(jnp.int32, (128, T), 0) == 0
    turned[...] = jnp.transpose(jnp.where(first_row, slot_row, gate[...]))
    slot_col = turned[:, 0:1]
    col = lax.broadcasted_iota(jnp.int32, (T, pair), 1).astype(f32)
    here = slot_col - (e * cap).astype(f32)
    there = slot_col - (partner * cap).astype(f32) + float(cap)
    pk[...] = (((col == here) & (col < cap)) | ((col == there) & (col >= cap))).astype(f32).astype(bf16)

    locals_[1].wait()
    d1_copy.wait_recv()
    for i in range(4):
        hidden(lambda: arrived[0:pair, :], pair, ein, *part_of(i, 4))
        if i == 1:
            for q in units:
                gather(q, 0)

    locals_[2].wait()

    def own_step(i, carry):
        cols = pl.ds(pl.multiple_of(i * 256, 256), 256)
        acc = jnp.dot(hbuf[0:pair, :], eout[:, cols], preferred_element_type=f32).astype(bf16)
        pown[0:cap, cols] = acc[0:cap, :]
        psend[:, cols] = acc[cap:pair, :]
        return carry

    own_blocks = D // 256
    lax.fori_loop(0, own_blocks // 2, own_step, 0)
    if Z > 2:
        for q in units:
            gather(q, 1)
    relay(EARLY)
    lax.fori_loop(own_blocks // 2, own_blocks, own_step, 0)

    @when(z == 0)
    def _():
        rpo[0] = jnp.zeros(rpo.shape[1:], bf16)
        rpd[0] = jnp.zeros(rpd.shape[1:], bf16)

    @when(z == Z - 1)
    def _():
        rpo[Z] = jnp.zeros(rpo.shape[1:], bf16)
        rpd[Z] = jnp.zeros(rpd.shape[1:], bf16)

    pq_copy = remote(psend, pown.at[pl.ds(cap, cap), :], pq_s.at[0], pq_r.at[0], ee=partner)
    pq_copy.start()

    def zo_copy(q, d, slot, to):
        rows = pl.ds((q - 2) * cap, cap)
        return remote(po.at[d, rows, :], rpo.at[slot, rows, :], zo_s.at[q, d], zo_r.at[q, slot], zz=to)

    def back_slot(d, to):
        return Z if d == to else d

    def zo_edge(q, i):
        @when(z == 0)
        def _():
            zo_copy(q, Z - 1 - i, Z - 1 - i, 1).start()

        @when(z == Z - 1)
        def _():
            zo_copy(q, i, back_slot(i, Z - 2), Z - 2).start()

    def expert_hidden(q):
        if q in fast:
            for at, s in ends:
                @when(z == at)
                def _():
                    dx_copy(q, 1, s).wait_recv()
        hidden(lambda: arrived[q * cap:(q + 1) * cap, :], cap, ein)

    def expert_out(q, between=None):
        rows = slice((q - 2) * cap, (q - 1) * cap)
        for i in range(Z):
            d = (1 - upper) * (Z - 1 - i) + upper * i

            def step(k, carry):
                acc = jnp.dot(hbuf[0:cap, :], eout[:, pl.ds(pl.multiple_of(d * share + k * 256, 256), 256)],
                              preferred_element_type=f32)
                po[d, rows, pl.ds(pl.multiple_of(k * 256, 256), 256)] = acc.astype(bf16)
                return carry

            lax.fori_loop(0, share // 256, step, 0)
            if i > 0:
                zo_edge(q, i - 1)
            if between is not None and i == Z // 2 - 1:
                between()

    def zo_up(q, d):
        @when((z > 0) & (z < d))
        def _():
            rows = slice((q - 2) * cap, (q - 1) * cap)
            zo_copy(q, d, d, above).wait_recv()
            po[d, rows, :] = (po[d, rows, :].astype(f32) + rpo[d, rows, :].astype(f32)).astype(bf16)
            zo_copy(q, d, d, above).start()

    def zo_down(q, d):
        @when((z < Z - 1) & (z > d))
        def _():
            rows = slice((q - 2) * cap, (q - 1) * cap)
            zo_copy(q, d, d, below).wait_recv()
            po[d, rows, :] = (po[d, rows, :].astype(f32) + rpo[d, rows, :].astype(f32)).astype(bf16)

        for slot, near in ((d, z > d + 1), (Z, z == d + 1)):
            @when((z < Z - 1) & near)
            def _():
                zo_copy(q, d, slot, below).start()

    def zo_near(q, t):
        @when(upper == 0)
        def _():
            zo_up(q, Z - 1 - t)

        @when(upper == 1)
        def _():
            zo_down(q, t)

    def zo_far(q, t):
        @when(upper == 0)
        def _():
            zo_down(q, t)

        @when(upper == 1)
        def _():
            zo_up(q, Z - 1 - t)

    def ret_copy(q):
        rows = pl.ds((q - 2) * cap, cap)
        return remote(ret.at[rows, :], rret.at[rows, :], ret_s.at[q], ret_r.at[q], ee=expert_at(-(q // 2), q % 2))

    def zo_final(q):
        @when(z > 0)
        def _():
            zo_copy(q, z, z, above).wait_recv()

        @when(z < Z - 1)
        def _():
            zo_copy(q, z, Z, above).wait_recv()
        rows = slice((q - 2) * cap, (q - 1) * cap)
        ret[rows, :] = (po[z, rows, :].astype(f32) + rpo[z, rows, :].astype(f32)
                        + rpo[Z, rows, :].astype(f32)).astype(bf16)

    def point(n):
        return n * SUBS[0] // 8 if n <= 8 else SUBS[0] + (n - 8) * SUBS[1] // 8

    def weights(to_take, to_relay):
        take(point(to_take))
        relay(point(to_relay))

    def passes(kind, group, t):
        if t < Z - 1:
            for q in group:
                kind(q, t)

    for t in range(2, Z - 1):
        for q in fast:
            gather(q, t)
    take(point(2))
    for n, q in enumerate(fast):
        expert_hidden(q)
        if n == len(fast) - 1:
            for k in slow:
                for t in range(2, Z - 1):
                    gather(k, t)
        expert_out(q)
    weights(4, 2)
    for n, q in enumerate(slow):
        gather(q, Z - 1)
        if n == 0:
            take(point(5))
        expert_hidden(q)
        if n == len(slow) - 1:
            weights(6, 3)
        expert_out(q, (lambda: weights(7, 5)) if n == len(slow) - 1 else None)
    weights(8, 6)
    passes(zo_near, fast, 0)
    passes(zo_far, fast, 0)
    passes(zo_near, fast, 1)
    weights(9, 8)
    passes(zo_far, fast, 1)
    for t in range(2, Z - 1):
        passes(zo_near, fast, t)
        passes(zo_far, fast, t)
    locals_[3].wait()
    own_copies[0].wait_recv()
    collect(0, range(SUBS[0]))

    def mlp_hidden(i):
        hidden(lambda: normed[...], T, win, *part_of(i, 4))

    mlp_hidden(0)
    weights(10, 8)
    mlp_hidden(1)
    weights(11, 9)
    mlp_hidden(2)
    passes(zo_near, slow, 0)
    mlp_hidden(3)
    weights(12, 10)

    def zd_copy(d, slot, c, to):
        cols = pl.ds(c * wide, wide)
        return remote(pd.at[d, :, cols], rpd.at[slot, :, cols], zd_s.at[d, c], zd_r.at[slot, c], zz=to)

    locals_[4].wait()
    own_copies[1].wait_recv()
    pq_copy.wait_recv()
    mine = Z // C if Z % C == 0 else 0

    def slice_number(i):
        if C == 2 and Z % 2 == 0:
            low = i if i < mine else Z - 1 - (i - mine)
            return chip * (Z - 1 - low) + (1 - chip) * low
        return lax.rem(chip * mine + i, Z)

    def late(i, c):
        return c == nk - 1 and nk > 1 and i == 1 and mine > 1

    def dense(i, c):
        d = slice_number(i)

        def step(k, carry):
            cols = pl.ds(pl.multiple_of(d * share + c * wide + k * tn, tn), tn)
            acc = jnp.dot(hbuf[0:T, :], wout[:, cols], preferred_element_type=f32)
            res = jnp.dot(pk[...], pown[:, cols], preferred_element_type=f32)
            pd[d, :, pl.ds(pl.multiple_of(c * wide + k * tn, tn), tn)] = (acc + turned[:, 1:2] * res).astype(bf16)
            return carry

        lax.fori_loop(0, wide // tn, step, 0)

        dense_edge(i, c, False)

    def dense_edge(i, c, again):
        d = slice_number(i)
        beside = ((z == 0) & (d == 1)) | ((z == Z - 1) & (d == Z - 2))
        go = (beside if again else ~beside) if late(i, c) else True
        if again and not late(i, c):
            return

        @when((z == 0) & (d > 0) & go)
        def _():
            zd_copy(d, d, c, above).start()

        for slot, near in ((d, z > d + 1), (Z, z == d + 1)):
            @when((z == Z - 1) & near & go)
            def _():
                zd_copy(d, slot, c, below).start()

    def zd_pass(i, c):
        d = slice_number(i)
        cols = pl.ds(c * wide, wide)

        @when((z > 0) & (z < Z - 1) & (z != d))
        def _():
            zd_copy(d, d, c, above).wait_recv()
            pd[d, :, cols] = (pd[d, :, cols].astype(f32) + rpd[d, :, cols].astype(f32)).astype(bf16)

        @when((z > 0) & (z < d))
        def _():
            zd_copy(d, d, c, above).start()

        for slot, near in ((d, z > d + 1), (Z, z == d + 1)):
            @when((z < Z - 1) & near)
            def _():
                zd_copy(d, slot, c, below).start()

    trow = min(128, T)
    residual = slice_at(z)

    def combine_experts():
        for q in units:
            ret_copy(q).wait_recv()
        for i in range(T // trow):
            rows = slice(i * trow, (i + 1) * trow)
            res = jnp.zeros((trow, share), f32)
            for q in units:
                wanted = turned[rows, 0:1] - (expert_at(q // 2, q % 2) * cap).astype(f32)
                pick = (lax.broadcasted_iota(jnp.int32, (trow, cap), 1).astype(f32) == wanted)
                res = res + jnp.dot(pick.astype(f32).astype(bf16), rret[(q - 2) * cap:(q - 1) * cap, :],
                                    preferred_element_type=f32)
            base[rows, :] = tok[rows, residual].astype(f32) + turned[rows, 1:2] * res

    def sent():
        for copy in own_copies:
            copy.wait_send()
        d1_copy.wait_send()
        pq_copy.wait_send()
        for q in units:
            dx_copy(q, 0, z).wait_send()
            ret_copy(q).wait_send()
            for at, s in ends:
                @when((z == at) & (q in fast))
                def _():
                    dx_copy(q, 1, s).wait_send()
            for t in range(1, hops(q) + 1):
                @when((z >= t - 1) & (z < Z - 1))
                def _():
                    hop(q, 0, t, z - t + 1).wait_send()

                @when((z + t - 1 <= Z - 1) & (z > 0))
                def _():
                    hop(q, 1, t, z + t - 1).wait_send()
        for m in range(2):
            for s in range(SUBS[m]):
                for kc in range(1, C):
                    x_copy(m, kc, s).wait_send()
                    for dg in range(1, G):
                        y_copy(m, kc, s, dg).wait_send()
                    for dg in range(G):
                        p_copy(m, kc, s, dg).wait_send()

    def finish(c):
        cols = slice(c * wide, (c + 1) * wide)

        @when(z > 0)
        def _():
            zd_copy(z, z, c, above).wait_recv()

        @when(z < Z - 1)
        def _():
            zd_copy(z, Z, c, above).wait_recv()

        for i in range(T // trow):
            rows = slice(i * trow, (i + 1) * trow)
            total = pd[z, rows, cols].astype(f32) + rpd[z, rows, cols].astype(f32) + rpd[Z, rows, cols].astype(f32)
            out[rows, cols] = (base[rows, cols] + total).astype(bf16)

    per = SUBS[1] // nk
    for c in range(nk):
        for i in range(mine):
            dense(i, c)
        if c == 0:
            weights(13, 11)
            passes(zo_near, slow, 1)
            passes(zo_far, slow, 0)
            passes(zo_far, slow, 1)
            for t in range(2, Z - 1):
                passes(zo_near, slow, t)
                passes(zo_far, slow, t)
            for q in fast:
                zo_final(q)
                ret_copy(q).start()
    for c in range(nk):
        if c == nk - 1:
            weights(15, 13)
            weights(16, 14)
            weights(16, 15)
            weights(16, 16)
        else:
            weights(14, 12)
        collect(1, range(c * per, (c + 1) * per))
        for i in range(mine, Z):
            dense(i, c)
        if c == 0:
            for q in slow:
                zo_final(q)
                ret_copy(q).start()
    for c in range(nk):
        for i in range(Z):
            dense_edge(i, c, True)
    low_first = list(range(Z)) if mine == 0 else list(range(mine, Z)) + list(range(mine))
    turn = lax.rem(upper + chip, 2) if C == 2 else upper
    for c in range(nk):
        for flag, order in ((0, low_first), (1, list(range(Z)))):
            @when(turn == flag)
            def _():
                for i in order if C == 2 else range(Z):
                    zd_pass(i, c)
        if c == 0:
            combine_experts()
            sent()
    for c in range(nk):
        finish(c)

    for d in range(Z):
        @when(z != d)
        def _():
            for q in units:
                zo_copy(q, d, d, above).wait_send()
            for c in range(nk):
                zd_copy(d, d, c, above).wait_send()


def local(tokens, route, gate_prob, norm_gain, dense_in, dense_out, expert_in, expert_out):
    G, E, Z = lax.axis_size("groups"), lax.axis_size("expert"), lax.axis_size("cuts")
    T, D = tokens.shape
    F = dense_in.shape[1]
    share = D // Z
    De = D // E
    cap = max(2, 3 * T // (2 * E))
    C = E // 2
    others = (E - 2) * cap
    nk = 2 if De == share and share % 256 == 0 else 1
    bf16 = jnp.bfloat16
    any_, vmem = pl.BlockSpec(memory_space=pl.ANY), pl.BlockSpec(memory_space=pltpu.VMEM)
    dma = pltpu.SemaphoreType.DMA
    splits = (max(1, min(8, De // (16 * G))), 8)
    subs = max(splits)
    return pl.pallas_call(
        functools.partial(kernel, G, E, Z, cap, nk, splits),
        out_shape=jax.ShapeDtypeStruct((T, share), bf16),
        in_specs=[any_, vmem, vmem, vmem, any_, any_, any_, any_],
        out_specs=vmem,
        scratch_shapes=[
            pltpu.VMEM((D, F), bf16), pltpu.VMEM((F, D), bf16),
            pltpu.VMEM((D, F), bf16), pltpu.VMEM((F, D), bf16),
            pltpu.VMEM((T, D), bf16), pltpu.VMEM((T, D), bf16),
            pltpu.VMEM((2, others, share), bf16), pltpu.VMEM((cap, D), bf16), pltpu.VMEM((E * cap, D), bf16),
            pltpu.VMEM((max(T, 2 * cap), F), bf16),
            pltpu.VMEM((2 * cap, D), bf16), pltpu.VMEM((cap, D), bf16),
            pltpu.VMEM((Z, others, share), bf16), pltpu.VMEM((Z + 1, others, share), bf16),
            pltpu.VMEM((Z, T, share), bf16), pltpu.VMEM((Z + 1, T, share), bf16),
            pltpu.VMEM((others, share), bf16), pltpu.VMEM((others, share), bf16),
            pltpu.VMEM((T, share), jnp.float32), pltpu.VMEM((T, 2 * cap), bf16),
            pltpu.VMEM((T, 128), jnp.float32),
            dma((5,)), dma((2,)), dma((2,)), dma((1,)), dma((1,)), dma((E, 2)), dma((E, 2)),
            dma((E, 2, Z)), dma((E, 2, Z)), dma((1,)), dma((1,)),
            dma((2, C, subs)), dma((2, C, subs)),
            dma((2, C, subs, G)), dma((2, C, subs, G)), dma((2, C, subs, G)), dma((2, C, subs, G)),
            dma((E, Z)), dma((E, Z + 1)), dma((Z, nk)), dma((Z + 1, nk)), dma((E,)), dma((E,)),
        ],
        compiler_params=pltpu.CompilerParams(
            collective_id=0, has_side_effects=True, vmem_limit_bytes=67043328
        ),
    )(tokens, route.reshape(1, T), gate_prob[None, :], norm_gain[None, :], dense_in, dense_out, expert_in, expert_out)


def solution(mesh):
    return jax.shard_map(
        local,
        mesh=mesh,
        in_specs=(
            P(("groups", "expert"), None),
            P(("groups", "expert"), None),
            P(("groups", "expert")),
            P(),
            P("expert", "cuts"),
            P("cuts", "expert"),
            P("expert", None, "cuts"),
            P("expert", "cuts", None),
        ),
        out_specs=P(("groups", "expert"), "cuts"),
        check_vma=False,
    )
```

```python
import functools

import jax
import jax.numpy as jnp
from jax import lax
from jax.experimental import pallas as pl
from jax.experimental.pallas import tpu as pltpu
from jax.sharding import PartitionSpec as P

EARLY = 1


def kernel(G, E, Z, cap, nk, SUBS, tokens, route, gate, gain, din, dout, ein_h, eout_h, out,
           win, wout, ein, eout, tok, normed, disp, dispq, arrived, hbuf, pown, psend, po, rpo, pd, rpd,
           ret, rret, base, pk, turned, eres,
           loc, own_s, own_r, d1_s, d1_r, dx_s, dx_r, ag_s, ag_r, pq_s, pq_r,
           wx_s, wx_r, wy_s, wy_r, wp_s, wp_r, zo_s, zo_r, zd_s, zd_r, ret_s, ret_r):
    f32, bf16 = jnp.float32, jnp.bfloat16
    T, D = tok.shape
    F = ein.shape[1]
    De = D // E
    share = D // Z
    C = E // 2
    wide = share // nk
    tn = min(256, wide)
    units = range(2, E)
    fast, slow = units[:(E - 2) // 2], units[(E - 2) // 2:]
    g, e, z = lax.axis_index("groups"), lax.axis_index("expert"), lax.axis_index("cuts")
    chip, core = e // 2, lax.rem(e, 2)
    partner = chip * 2 + 1 - core
    above, below = lax.rem(z + 1, Z), lax.rem(z + Z - 1, Z)
    upper = (2 * z) // Z

    def remote(src, dst, send, recv, gg=None, ee=None, zz=None):
        return pltpu.make_async_remote_copy(
            src_ref=src, dst_ref=dst, send_sem=send, recv_sem=recv,
            device_id={
                "groups": g if gg is None else gg,
                "expert": e if ee is None else ee,
                "cuts": z if zz is None else zz,
            },
            device_id_type=pl.DeviceIdType.MESH,
        )

    def when(condition):
        return pl.when(condition)

    def expert_at(kc, j):
        other = lax.rem(chip + kc + C, C)
        return other * 2 + (core if j == 0 else 1 - core)

    my_rows = pl.ds(pl.multiple_of(e * De, De), De)
    locals_ = [
        pltpu.make_async_copy(tokens, tok, loc.at[0]),
        pltpu.make_async_copy(ein_h.at[0], ein, loc.at[1]),
        pltpu.make_async_copy(eout_h.at[0], eout, loc.at[2]),
        pltpu.make_async_copy(din, win.at[my_rows, :], loc.at[3]),
        pltpu.make_async_copy(dout, wout.at[:, my_rows], loc.at[4]),
    ]
    locals_[0].start()

    barrier = pltpu.get_barrier_semaphore()
    for k in range(1, E):
        pl.semaphore_signal(barrier, inc=1, device_id={"groups": g, "expert": lax.rem(e + k, E), "cuts": z},
                            device_id_type=pl.DeviceIdType.MESH)
    for k in range(1, Z):
        pl.semaphore_signal(barrier, inc=1, device_id={"groups": g, "expert": e, "cuts": lax.rem(z + k, Z)},
                            device_id_type=pl.DeviceIdType.MESH)
    for k in range(1, G):
        pl.semaphore_signal(barrier, inc=1, device_id={"groups": lax.rem(g + k, G), "expert": e, "cuts": z},
                            device_id_type=pl.DeviceIdType.MESH)
    pl.semaphore_wait(barrier, (E - 1) + (Z - 1) + (G - 1))

    own_copies = [
        remote(din, win.at[my_rows, :], own_s.at[0], own_r.at[0], ee=partner),
        remote(dout, wout.at[:, my_rows], own_s.at[1], own_r.at[1], ee=partner),
    ]

    def block(m, p, s):
        if m == 0:
            n = De // G // SUBS[0]
            return p * (De // G) + s * n, n, 0, F
        per = SUBS[1] // nk
        n = F // G // per
        return p * (F // G) + (s % per) * n, n, (s // per) * (De // nk), De // nk

    def weight(m, owner, p, s):
        row, n, col, width = block(m, p, s)
        if m == 0:
            return win.at[pl.ds(pl.multiple_of(owner * De + row, n), n), :]
        return wout.at[pl.ds(pl.multiple_of(row, n), n),
                       pl.ds(pl.multiple_of(owner * De + col, width), width)]

    def weight_source(m, p, s):
        row, n, col, width = block(m, p, s)
        return (din, dout)[m].at[pl.ds(pl.multiple_of(row, n), n), pl.ds(col, width)]

    def x_copy(m, kc, s):
        return remote(weight_source(m, g, s), weight(m, e, g, s), wx_s.at[m], wx_r.at[m, kc - 1, s],
                      ee=expert_at(kc, 0))

    def y_copy(m, kc, s, dg):
        w = weight(m, expert_at(-kc, 0), g, s)
        return remote(w, w, wy_s.at[m], wy_r.at[m, kc - 1, s, dg - 1], gg=lax.rem(g + dg, G))

    def p_copy(m, kc, s, dg):
        w = weight(m, expert_at(-kc, 0), lax.rem(g - dg + G, G), s)
        return remote(w, w, wp_s.at[m], wp_r.at[m * (1 + s // (SUBS[1] // nk))], ee=partner)

    steps = [(m, s) for m in range(2) for s in range(SUBS[m])]
    issued, taken, relayed = [0], [0], [0]

    def issue(upto):
        while issued[0] < min(upto, len(steps)):
            m, s = steps[issued[0]]
            for kc in range(1, C):
                x_copy(m, kc, s).start()
            issued[0] += 1

    def relay(upto):
        while relayed[0] < min(upto, taken[0]):
            m, s = steps[relayed[0]]
            for kc in range(1, C):
                for dg in range(1, G):
                    y_copy(m, kc, s, dg).wait_recv()
                    p_copy(m, kc, s, dg).start()
            relayed[0] += 1

    def take(upto):
        while taken[0] < min(upto, len(steps)):
            m, s = steps[taken[0]]
            for kc in range(1, C):
                x_copy(m, kc, s).wait_recv()
                for dg in range(1, G):
                    y_copy(m, kc, s, dg).start()
                p_copy(m, kc, s, 0).start()
            taken[0] += 1

    def weight_part(m, rows, cols):
        return (win, wout)[m].at[pl.ds(0, rows), pl.ds(0, cols)]

    def collect(n):
        w = weight_part(1, F, (C - 1) * De // nk) if n else weight_part(0, (C - 1) * De, F)
        remote(w, w, wp_s.at[0], wp_r.at[n], ee=partner).wait_recv()

    issue(EARLY)
    locals_[0].wait()
    for copy in locals_[1:]:
        copy.start()

    nrow = min(64, T)

    def norm_step(i, carry):
        rows = pl.ds(pl.multiple_of(i * nrow, nrow), nrow)
        x = tok[rows, :].astype(f32)
        ms = jnp.mean(x * x, axis=-1, keepdims=True)
        normed[rows, :] = (x * lax.rsqrt(ms + 1e-06) * gain[...]).astype(bf16)
        return carry

    lax.fori_loop(0, T // nrow, norm_step, 0)

    picked = route[...]
    lanes = -(-E // 8) * 8
    one_hot = (lax.broadcasted_iota(jnp.int32, (lanes, T), 0) == picked).astype(f32)
    earlier = (lax.broadcasted_iota(jnp.int32, (T, T), 0) < lax.broadcasted_iota(jnp.int32, (T, T), 1))
    before = jnp.dot(one_hot.astype(bf16), earlier.astype(f32).astype(bf16), preferred_element_type=f32)
    position = jnp.sum(before * one_hot, axis=0, keepdims=True)
    slot_row = picked.astype(f32) * float(cap) + position

    def slice_at(s):
        return pl.ds(pl.multiple_of(s * share, share), share)

    def picks(q):
        dest = expert_at(q // 2, q % 2)
        wanted = slot_row - (dest * cap).astype(f32)
        return (lax.broadcasted_iota(jnp.int32, (cap, T), 0).astype(f32) == wanted).astype(f32).astype(bf16)

    def fill_slice(q, x, s):
        disp[x, (q - 2) * cap:(q - 1) * cap, :] = jnp.dot(
            picks(q), normed[:, slice_at(s)], preferred_element_type=f32).astype(bf16)

    def fill(q, dst):
        pick = picks(q)
        dn = min(512, D)

        def step(i, carry):
            cols = pl.ds(pl.multiple_of(i * dn, dn), dn)
            dst[0:cap, cols] = jnp.dot(pick, normed[:, cols], preferred_element_type=f32).astype(bf16)
            return carry

        lax.fori_loop(0, D // dn, step, 0)

    ends = ((0, Z - 1), (Z - 1, 0))

    def dx_copy(q, x, s):
        return remote(disp.at[x, pl.ds((q - 2) * cap, cap), :], arrived.at[pl.ds(q * cap, cap), slice_at(s)],
                      dx_s.at[q - 2, x], dx_r.at[q - 2, x], ee=expert_at(q // 2, q % 2))

    d1_copy = remote(dispq, arrived.at[pl.ds(cap, cap), :], d1_s.at[0], d1_r.at[0], ee=partner)

    pending = None
    for q in units:
        fill_slice(q, 0, z)
        if pending is not None:
            dx_copy(pending, 0, z).start()
        pending = q
    for at, s in ends:
        @when(z == at)
        def _():
            for q in fast:
                fill_slice(q, 1, s)
    if pending is not None:
        dx_copy(pending, 0, z).start()
    fill(1, dispq)
    for at, s in ends:
        @when(z == at)
        def _():
            for q in fast:
                dx_copy(q, 1, s).start()
    issue(len(steps))
    fill(0, arrived)
    d1_copy.start()
    for copy in own_copies:
        copy.start()

    def hop(q, way, t, s):
        part = arrived.at[pl.ds(q * cap, cap), slice_at(s)]
        return remote(part, part, ag_s.at[q - 2, way, t - 1], ag_r.at[q - 2, way, t - 1], zz=below if way else above)

    def hops(q):
        return Z - 2 if q in fast else Z - 1

    def gather(q, t):
        if t == 0:
            dx_copy(q, 0, z).wait_recv()

        @when(z >= t)
        def _():
            if t > 0:
                hop(q, 0, t, z - t).wait_recv()
        if t < hops(q):
            @when((z >= t) & (z < Z - 1))
            def _():
                hop(q, 0, t + 1, z - t).start()

        @when(z + t <= Z - 1)
        def _():
            if t > 0:
                hop(q, 1, t, z + t).wait_recv()
        if t < hops(q):
            @when((z + t <= Z - 1) & (z > 0))
            def _():
                hop(q, 1, t + 1, z + t).start()

    def hidden(load, rows, w, lo=0, hi=None):
        def step(i, carry):
            cols = pl.ds(pl.multiple_of(i * 256, 256), 256)
            acc = jnp.dot(load(), w[:, cols], preferred_element_type=f32)
            hbuf[0:rows, cols] = jax.nn.gelu(acc).astype(bf16)
            return carry

        lax.fori_loop(lo, F // 256 if hi is None else hi, step, 0)

    blocks = F // 256

    def part_of(i, n):
        return i * blocks // n, (i + 1) * blocks // n

    pair = 2 * cap
    take(EARLY)
    first_row = lax.broadcasted_iota(jnp.int32, (128, T), 0) == 0
    turned[...] = jnp.transpose(jnp.where(first_row, slot_row, gate[...]))
    slot_col = turned[:, 0:1]
    col = lax.broadcasted_iota(jnp.int32, (T, pair), 1).astype(f32)
    here = slot_col - (e * cap).astype(f32)
    there = slot_col - (partner * cap).astype(f32) + float(cap)
    pk[...] = (((col == here) & (col < cap)) | ((col == there) & (col >= cap))).astype(f32).astype(bf16)

    locals_[1].wait()
    d1_copy.wait_recv()
    for i in range(4):
        hidden(lambda: arrived[0:pair, :], pair, ein, *part_of(i, 4))
        if i == 1:
            for q in units:
                gather(q, 0)

    locals_[2].wait()

    def own_step(i, carry):
        cols = pl.ds(pl.multiple_of(i * 256, 256), 256)
        acc = jnp.dot(hbuf[0:pair, :], eout[:, cols], preferred_element_type=f32).astype(bf16)
        pown[0:cap, cols] = acc[0:cap, :]
        psend[:, cols] = acc[cap:pair, :]
        return carry

    own_blocks = D // 256
    lax.fori_loop(0, own_blocks // 2, own_step, 0)
    if Z > 2:
        for q in units:
            gather(q, 1)
    relay(EARLY)
    lax.fori_loop(own_blocks // 2, own_blocks, own_step, 0)

    @when(z == 0)
    def _():
        rpo[0] = jnp.zeros(rpo.shape[1:], bf16)
        rpd[0] = jnp.zeros(rpd.shape[1:], bf16)

    @when(z == Z - 1)
    def _():
        rpo[Z] = jnp.zeros(rpo.shape[1:], bf16)
        rpd[Z] = jnp.zeros(rpd.shape[1:], bf16)

    pq_copy = remote(psend, pown.at[pl.ds(cap, cap), :], pq_s.at[0], pq_r.at[0], ee=partner)
    pq_copy.start()

    def zo_copy(q, d, slot, to):
        rows = pl.ds((q - 2) * cap, cap)
        return remote(po.at[d, rows, :], rpo.at[slot, rows, :], zo_s.at[0], zo_r.at[q - 2, slot], zz=to)

    def back_slot(d, to):
        return Z if d == to else d

    def zo_edge(q, i):
        @when(z == 0)
        def _():
            zo_copy(q, Z - 1 - i, Z - 1 - i, 1).start()

        @when(z == Z - 1)
        def _():
            zo_copy(q, i, back_slot(i, Z - 2), Z - 2).start()

    def expert_hidden(q, between=None):
        if q in fast:
            for at, s in ends:
                @when(z == at)
                def _():
                    dx_copy(q, 1, s).wait_recv()
        rows = slice(q * cap, (q + 1) * cap)
        hidden(lambda: arrived[rows, :], cap, ein, *part_of(0, 2))
        if between is not None:
            between()
        hidden(lambda: arrived[rows, :], cap, ein, *part_of(1, 2))

    def expert_out(q, between=None):
        rows = slice((q - 2) * cap, (q - 1) * cap)
        for i in range(Z):
            d = (1 - upper) * (Z - 1 - i) + upper * i

            def step(k, carry):
                acc = jnp.dot(hbuf[0:cap, :], eout[:, pl.ds(pl.multiple_of(d * share + k * 256, 256), 256)],
                              preferred_element_type=f32)
                po[d, rows, pl.ds(pl.multiple_of(k * 256, 256), 256)] = acc.astype(bf16)
                return carry

            lax.fori_loop(0, share // 256, step, 0)
            if i > 0:
                zo_edge(q, i - 1)
            if between is not None:
                between(i)

    def zo_up(q, d):
        @when((z > 0) & (z < d))
        def _():
            rows = slice((q - 2) * cap, (q - 1) * cap)
            zo_copy(q, d, d, above).wait_recv()
            po[d, rows, :] = (po[d, rows, :].astype(f32) + rpo[d, rows, :].astype(f32)).astype(bf16)
            zo_copy(q, d, d, above).start()

    def zo_down(q, d):
        @when((z < Z - 1) & (z > d))
        def _():
            rows = slice((q - 2) * cap, (q - 1) * cap)
            zo_copy(q, d, d, below).wait_recv()
            po[d, rows, :] = (po[d, rows, :].astype(f32) + rpo[d, rows, :].astype(f32)).astype(bf16)

        for slot, near in ((d, z > d + 1), (Z, z == d + 1)):
            @when((z < Z - 1) & near)
            def _():
                zo_copy(q, d, slot, below).start()

    def zo_near(q, t):
        @when(upper == 0)
        def _():
            zo_up(q, Z - 1 - t)

        @when(upper == 1)
        def _():
            zo_down(q, t)

    def zo_far(q, t):
        @when(upper == 0)
        def _():
            zo_down(q, t)

        @when(upper == 1)
        def _():
            zo_up(q, Z - 1 - t)

    def ret_copy(q):
        rows = pl.ds((q - 2) * cap, cap)
        return remote(ret.at[rows, :], rret.at[rows, :], ret_s.at[q - 2], ret_r.at[q - 2], ee=expert_at(-(q // 2), q % 2))

    def zo_final(q):
        @when(z > 0)
        def _():
            zo_copy(q, z, z, above).wait_recv()

        @when(z < Z - 1)
        def _():
            zo_copy(q, z, Z, above).wait_recv()
        rows = slice((q - 2) * cap, (q - 1) * cap)
        ret[rows, :] = (po[z, rows, :].astype(f32) + rpo[z, rows, :].astype(f32)
                        + rpo[Z, rows, :].astype(f32)).astype(bf16)

    def point(n):
        return n * SUBS[0] // 8 if n <= 8 else SUBS[0] + (n - 8) * SUBS[1] // 8

    def weights(to_take, to_relay):
        take(point(to_take))
        relay(point(to_relay))

    def passes(kind, group, t):
        if t < Z - 1:
            for q in group:
                kind(q, t)

    for t in range(2, Z - 1):
        for q in fast:
            gather(q, t)
    take(point(2))
    for n, q in enumerate(fast):
        final = n == len(fast) - 1
        expert_hidden(q, (lambda: take(point(3))) if final else None)
        if final:
            for k in slow:
                for t in range(2, Z - 1):
                    gather(k, t)
        expert_out(q, (lambda i: take(point(4))) if final else None)
    weights(5, 2)
    pq_copy.wait_recv()

    def own_rows(i, carry):
        cols = pl.ds(pl.multiple_of(i * 256, 256), 256)
        res = jnp.dot(pk[...], pown[:, cols], preferred_element_type=f32)
        eres[:, cols] = (turned[:, 1:2] * res).astype(bf16)
        return carry

    lax.fori_loop(0, own_blocks, own_rows, 0)

    def serve(i):
        if i == Z // 2 - 1:
            relay(point(5))
            passes(zo_near, fast, 0)
        if i == Z // 2:
            weights(8, 6)

    for n, q in enumerate(slow):
        final = n == len(slow) - 1
        gather(q, Z - 1)
        if n == 0:
            weights(6, 3)
        expert_hidden(q, (lambda: weights(7, 4)) if final else None)
        expert_out(q, serve if final else None)
    passes(zo_near, fast, 1)
    weights(9, 7)
    passes(zo_far, fast, 0)
    relay(point(8))
    take(point(10))
    locals_[3].wait()
    own_copies[0].wait_recv()
    collect(0)

    def mlp_hidden(i):
        hidden(lambda: normed[...], T, win, *part_of(i, 4))

    mlp_hidden(0)
    weights(11, 9)
    mlp_hidden(1)
    take(point(12))
    passes(zo_far, fast, 1)
    for t in range(2, Z - 1):
        passes(zo_near, fast, t)
        passes(zo_far, fast, t)
    mlp_hidden(2)
    relay(point(10))
    passes(zo_near, slow, 0)
    mlp_hidden(3)
    weights(13, 11)

    nr = 2 if T % 32 == 0 else 1
    tall = T // nr
    halves = range(nr)

    def zd_copy(d, slot, c, r, to):
        rows, cols = pl.ds(r * tall, tall), pl.ds(c * wide, wide)
        n = c * nr + r
        return remote(pd.at[d, rows, cols], rpd.at[slot, rows, cols], zd_s.at[0], zd_r.at[slot, n], zz=to)

    locals_[4].wait()
    own_copies[1].wait_recv()
    mine = Z // C if Z % C == 0 else 0
    lined = C == 2 and nk == 2 and mine > 1
    turn = lax.rem(upper + chip, 2)

    def slice_number(i):
        if C == 2 and Z % 2 == 0:
            low = i if i < mine else Z - 1 - (i - mine)
            return chip * (Z - 1 - low) + (1 - chip) * low
        return lax.rem(chip * mine + i, Z)

    def late(i, c):
        return c == nk - 1 and lined and i < mine

    def dense(i, c):
        d = slice_number(i)
        if lined and i < mine:
            d = turn * d + (1 - turn) * slice_number(mine - 1 - i)

        def step(k, carry):
            cols = pl.ds(pl.multiple_of(d * share + c * wide + k * tn, tn), tn)
            acc = jnp.dot(hbuf[0:T, :], wout[:, cols], preferred_element_type=f32)
            pd[d, :, pl.ds(pl.multiple_of(c * wide + k * tn, tn), tn)] = (acc + eres[:, cols].astype(f32)).astype(bf16)
            return carry

        lax.fori_loop(0, wide // tn, step, 0)

        dense_edge(i, c, False, d)

    def dense_edge(i, c, again, d):
        beside = ((z == 0) & (d == 1)) | ((z == Z - 1) & (d == Z - 2))
        go = (beside if again else ~beside) if late(i, c) else True
        if again and not late(i, c):
            return

        @when((z == 0) & (d > 0) & go)
        def _():
            for r in halves:
                zd_copy(d, d, c, r, above).start()

        for slot, near in ((d, z > d + 1), (Z, z == d + 1)):
            @when((z == Z - 1) & near & go)
            def _():
                for r in halves:
                    zd_copy(d, slot, c, r, below).start()

    def zd_pass(i, c):
        d = slice_number(i)
        cols = pl.ds(c * wide, wide)
        for r in halves:
            rows = pl.ds(r * tall, tall)

            @when((z > 0) & (z < Z - 1) & (z != d))
            def _():
                zd_copy(d, d, c, r, above).wait_recv()
                pd[d, rows, cols] = (pd[d, rows, cols].astype(f32) + rpd[d, rows, cols].astype(f32)).astype(bf16)

            @when((z > 0) & (z < d))
            def _():
                zd_copy(d, d, c, r, above).start()

            for slot, near in ((d, z > d + 1), (Z, z == d + 1)):
                @when((z < Z - 1) & near)
                def _():
                    zd_copy(d, slot, c, r, below).start()

    trow = min(128, T)
    residual = slice_at(z)

    def combine_experts():
        for q in units:
            ret_copy(q).wait_recv()
        for i in range(T // trow):
            rows = slice(i * trow, (i + 1) * trow)
            res = jnp.zeros((trow, share), f32)
            for q in units:
                wanted = turned[rows, 0:1] - (expert_at(q // 2, q % 2) * cap).astype(f32)
                pick = (lax.broadcasted_iota(jnp.int32, (trow, cap), 1).astype(f32) == wanted)
                res = res + jnp.dot(pick.astype(f32).astype(bf16), rret[(q - 2) * cap:(q - 1) * cap, :],
                                    preferred_element_type=f32)
            base[rows, :] = tok[rows, residual].astype(f32) + turned[rows, 1:2] * res

    def sent():
        for copy in own_copies:
            copy.wait_send()
        d1_copy.wait_send()
        pq_copy.wait_send()
        for q in units:
            dx_copy(q, 0, z).wait_send()
            ret_copy(q).wait_send()
            for at, s in ends:
                @when((z == at) & (q in fast))
                def _():
                    dx_copy(q, 1, s).wait_send()
            for t in range(1, hops(q) + 1):
                @when((z >= t - 1) & (z < Z - 1))
                def _():
                    hop(q, 0, t, z - t + 1).wait_send()

                @when((z + t - 1 <= Z - 1) & (z > 0))
                def _():
                    hop(q, 1, t, z + t - 1).wait_send()
        for m in range(2):
            for sem, n in ((wx_s, 1), (wy_s, G - 1), (wp_s, G)):
                rows, cols = ((C - 1) * De // G * n, F) if m == 0 else (F // G * n, (C - 1) * De)
                w = weight_part(m, rows, cols)
                remote(w, w, sem.at[m], wp_r.at[0], ee=partner).wait_send()

    def finish(c):
        cols = slice(c * wide, (c + 1) * wide)

        for r in halves:
            @when(z > 0)
            def _():
                zd_copy(z, z, c, r, above).wait_recv()

            @when(z < Z - 1)
            def _():
                zd_copy(z, Z, c, r, above).wait_recv()

        for i in range(T // trow):
            rows = slice(i * trow, (i + 1) * trow)
            total = pd[z, rows, cols].astype(f32) + rpd[z, rows, cols].astype(f32) + rpd[Z, rows, cols].astype(f32)
            out[rows, cols] = (base[rows, cols] + total).astype(bf16)

    per = SUBS[1] // nk
    def along(kind):
        for i, c in kind:
            zd_pass(i, c)

    def in_turn(first_kind, second_kind):
        @when(turn == 0)
        def _():
            along(first_kind)

        @when(turn == 1)
        def _():
            along(second_kind)

    near, far = list(range(mine, Z)), list(range(mine))

    for i in range(mine):
        dense(i, 0)
    weights(14, 12)
    passes(zo_near, slow, 1)
    passes(zo_far, slow, 0)
    if nk > 1:
        collect(1)
        for i in range(mine, Z):
            dense(i, 0)
        weights(15, 13)
        passes(zo_far, slow, 1)
        for q in fast:
            zo_final(q)
            ret_copy(q).start()
        for c in range(1, nk):
            for i in range(mine):
                dense(i, c)
    weights(16, 14)
    for t in range(1 if nk == 1 else 2, Z - 1):
        passes(zo_near, slow, t)
        passes(zo_far, slow, t)
    for q in slow if nk > 1 else units:
        zo_final(q)
        ret_copy(q).start()
    if lined:
        in_turn([], [(i, 0) for i in far[:1]])
    relay(point(15))
    relay(point(16))
    collect(nk)
    for i in range(mine, Z):
        dense(i, nk - 1)
    for c in range(nk):
        for i in range(Z):
            dense_edge(i, c, True, slice_number(i))
    if lined:
        in_turn([(near[0], 0)], [(i, 0) for i in far[1:]])
        combine_experts()
        in_turn([(i, 0) for i in far + near[1:]] + [(near[0], 1)],
                [(far[0], 1)] + [(i, 0) for i in near] + [(i, 1) for i in far[1:]])
        sent()
        in_turn([(i, 1) for i in far + near[1:]], [(i, 1) for i in near])
    else:
        for c in range(nk):
            along([(i, c) for i in range(Z)])
            if c == 0:
                combine_experts()
                sent()
    for c in range(nk):
        finish(c)

    def last_waits():
        for array, sem in ((po, zo_s), (pd, zd_s)):
            part = array.at[pl.ds(0, Z - 1)]
            remote(part, part, sem.at[0], wp_r.at[0], ee=partner).wait_send()

    last_waits()


def local(tokens, route, gate_prob, norm_gain, dense_in, dense_out, expert_in, expert_out):
    G, E, Z = lax.axis_size("groups"), lax.axis_size("expert"), lax.axis_size("cuts")
    T, D = tokens.shape
    F = dense_in.shape[1]
    share = D // Z
    De = D // E
    cap = max(2, 3 * T // (2 * E))
    C = E // 2
    away = E - 2
    others = away * cap
    nk = 2 if De == share and share % 256 == 0 else 1
    bf16 = jnp.bfloat16
    any_, vmem = pl.BlockSpec(memory_space=pl.ANY), pl.BlockSpec(memory_space=pltpu.VMEM)
    dma = pltpu.SemaphoreType.DMA
    splits = (max(1, min(8, De // (16 * G))), 8)
    subs = max(splits)
    return pl.pallas_call(
        functools.partial(kernel, G, E, Z, cap, nk, splits),
        out_shape=jax.ShapeDtypeStruct((T, share), bf16),
        in_specs=[any_, vmem, vmem, vmem, any_, any_, any_, any_],
        out_specs=vmem,
        scratch_shapes=[
            pltpu.VMEM((D, F), bf16), pltpu.VMEM((F, D), bf16),
            pltpu.VMEM((D, F), bf16), pltpu.VMEM((F, D), bf16),
            pltpu.VMEM((T, D), bf16), pltpu.VMEM((T, D), bf16),
            pltpu.VMEM((2, others, share), bf16), pltpu.VMEM((cap, D), bf16), pltpu.VMEM((E * cap, D), bf16),
            pltpu.VMEM((max(T, 2 * cap), F), bf16),
            pltpu.VMEM((2 * cap, D), bf16), pltpu.VMEM((cap, D), bf16),
            pltpu.VMEM((Z, others, share), bf16), pltpu.VMEM((Z + 1, others, share), bf16),
            pltpu.VMEM((Z, T, share), bf16), pltpu.VMEM((Z + 1, T, share), bf16),
            pltpu.VMEM((others, share), bf16), pltpu.VMEM((others, share), bf16),
            pltpu.VMEM((T, share), jnp.float32), pltpu.VMEM((T, 2 * cap), bf16),
            pltpu.VMEM((T, 128), jnp.float32), pltpu.VMEM((T, D), bf16),
            dma((5,)), dma((2,)), dma((2,)), dma((1,)), dma((1,)), dma((away, 2)), dma((away, 2)),
            dma((away, 2, Z - 1)), dma((away, 2, Z - 1)), dma((1,)), dma((1,)),
            dma((2,)), dma((2, C - 1, subs)), dma((2,)), dma((2, C - 1, subs, G - 1)), dma((2,)), dma((1 + nk,)),
            dma((1,)), dma((away, Z + 1)), dma((1,)), dma((Z + 1, 2 * nk)), dma((away,)), dma((away,)),
        ],
        compiler_params=pltpu.CompilerParams(
            collective_id=0, has_side_effects=True, vmem_limit_bytes=67043328
        ),
    )(tokens, route.reshape(1, T), gate_prob[None, :], norm_gain[None, :], dense_in, dense_out, expert_in, expert_out)


def solution(mesh):
    return jax.shard_map(
        local,
        mesh=mesh,
        in_specs=(
            P(("groups", "expert"), None),
            P(("groups", "expert"), None),
            P(("groups", "expert")),
            P(),
            P("expert", "cuts"),
            P("cuts", "expert"),
            P("expert", None, "cuts"),
            P("expert", "cuts", None),
        ),
        out_specs=P(("groups", "expert"), "cuts"),
        check_vma=False,
    )
```

```python
import functools

import jax
import jax.numpy as jnp
from jax import lax
from jax.experimental import pallas as pl
from jax.experimental.pallas import tpu as pltpu
from jax.sharding import PartitionSpec as P

EARLY = 1


def kernel(G, E, Z, cap, nk, SUBS, tokens, route_h, gate_h, gain_h, din, dout, ein_h, eout_h, out,
           win, wout, ein, eout, tok, normed, disp, dispq, arrived, hbuf, pown, psend, po, rpo, pd, rpd,
           ret, rret, base, pk, turned, eres, route, gate, gain,
           loc, own_s, own_r, d1_s, d1_r, dx_s, dx_r, ag_s, ag_r, pq_s, pq_r,
           wx_s, wx_r, wy_s, wy_r, wp_s, wp_r, zo_s, zo_r, zd_s, zd_r, ret_s, ret_r):
    f32, bf16 = jnp.float32, jnp.bfloat16
    T, D = tok.shape
    F = ein.shape[1]
    De = D // E
    share = D // Z
    C = E // 2
    wide = share // nk
    tn = min(256, wide)
    units = range(2, E)
    fast, slow = units[:(E - 2) // 2], units[(E - 2) // 2:]
    g, e, z = lax.axis_index("groups"), lax.axis_index("expert"), lax.axis_index("cuts")
    chip, core = e // 2, lax.rem(e, 2)
    partner = chip * 2 + 1 - core
    above, below = lax.rem(z + 1, Z), lax.rem(z + Z - 1, Z)
    upper = (2 * z) // Z

    def remote(src, dst, send, recv, gg=None, ee=None, zz=None):
        return pltpu.make_async_remote_copy(
            src_ref=src, dst_ref=dst, send_sem=send, recv_sem=recv,
            device_id={
                "groups": g if gg is None else gg,
                "expert": e if ee is None else ee,
                "cuts": z if zz is None else zz,
            },
            device_id_type=pl.DeviceIdType.MESH,
        )

    def when(condition):
        return pl.when(condition)

    def expert_at(kc, j):
        other = lax.rem(chip + kc + C, C)
        return other * 2 + (core if j == 0 else 1 - core)

    my_rows = pl.ds(pl.multiple_of(e * De, De), De)
    locals_ = [
        pltpu.make_async_copy(route_h, route, loc.at[0]),
        pltpu.make_async_copy(ein_h.at[0], ein, loc.at[1]),
        pltpu.make_async_copy(eout_h.at[0], eout, loc.at[2]),
        pltpu.make_async_copy(din, win.at[my_rows, :], loc.at[3]),
        pltpu.make_async_copy(dout, wout.at[:, my_rows], loc.at[4]),
    ]
    chunks = 4 if T % 256 == 0 else 1
    loads = []
    for k in range(chunks):
        part = pl.ds(k * (T // chunks), T // chunks)
        loads.append(pltpu.make_async_copy(tokens.at[part, :], tok.at[part, :], loc.at[5 + k]))
    small = [
        pltpu.make_async_copy(gain_h, gain, loc.at[9]),
        pltpu.make_async_copy(gate_h, gate, loc.at[10]),
        locals_[0],
    ]
    for copy in small + loads:
        copy.start()

    barrier = pltpu.get_barrier_semaphore()
    for k in range(1, E):
        pl.semaphore_signal(barrier, inc=1, device_id={"groups": g, "expert": lax.rem(e + k, E), "cuts": z},
                            device_id_type=pl.DeviceIdType.MESH)
    for k in range(1, Z):
        pl.semaphore_signal(barrier, inc=1, device_id={"groups": g, "expert": e, "cuts": lax.rem(z + k, Z)},
                            device_id_type=pl.DeviceIdType.MESH)
    for k in range(1, G):
        pl.semaphore_signal(barrier, inc=1, device_id={"groups": lax.rem(g + k, G), "expert": e, "cuts": z},
                            device_id_type=pl.DeviceIdType.MESH)
    pl.semaphore_wait(barrier, (E - 1) + (Z - 1) + (G - 1))

    own_copies = [
        remote(din, win.at[my_rows, :], own_s.at[0], own_r.at[0], ee=partner),
        remote(dout, wout.at[:, my_rows], own_s.at[1], own_r.at[1], ee=partner),
    ]

    def block(m, p, s):
        if m == 0:
            n = De // G // SUBS[0]
            return p * (De // G) + s * n, n, 0, F
        per = SUBS[1] // nk
        n = F // G // per
        return p * (F // G) + (s % per) * n, n, (s // per) * (De // nk), De // nk

    def weight(m, owner, p, s):
        row, n, col, width = block(m, p, s)
        if m == 0:
            return win.at[pl.ds(pl.multiple_of(owner * De + row, n), n), :]
        return wout.at[pl.ds(pl.multiple_of(row, n), n),
                       pl.ds(pl.multiple_of(owner * De + col, width), width)]

    def weight_source(m, p, s):
        row, n, col, width = block(m, p, s)
        return (din, dout)[m].at[pl.ds(pl.multiple_of(row, n), n), pl.ds(col, width)]

    def direct(m, s):
        return m == 0 and s == SUBS[0] - 1 and s > 0

    def x_copy(m, kc, s, dg=0):
        half = lax.rem(g - dg + G, G)
        return remote(weight_source(m, half, s), weight(m, e, half, s), wx_s.at[m],
                      wx_r.at[m, kc - 1, s + dg], ee=expert_at(kc, 0))

    def y_copy(m, kc, s, dg):
        w = weight(m, expert_at(-kc, 0), g, s)
        return remote(w, w, wy_s.at[m], wy_r.at[m, kc - 1, s, dg - 1], gg=lax.rem(g + dg, G))

    def p_copy(m, kc, s, dg):
        w = weight(m, expert_at(-kc, 0), lax.rem(g - dg + G, G), s)
        return remote(w, w, wp_s.at[m], wp_r.at[m * (1 + s // (SUBS[1] // nk))], ee=partner)

    steps = [(m, s) for m in range(2) for s in range(SUBS[m])]
    issued, taken, relayed = [0], [0], [0]

    def issue(upto):
        while issued[0] < min(upto, len(steps)):
            m, s = steps[issued[0]]
            for kc in range(1, C):
                for dg in range(G if direct(m, s) else 1):
                    x_copy(m, kc, s, dg).start()
            issued[0] += 1

    def relay(upto):
        while relayed[0] < min(upto, taken[0]):
            m, s = steps[relayed[0]]
            for kc in range(1, C):
                for dg in range(1, 1 if direct(m, s) else G):
                    y_copy(m, kc, s, dg).wait_recv()
                    p_copy(m, kc, s, dg).start()
            relayed[0] += 1

    def take(upto):
        while taken[0] < min(upto, len(steps)):
            m, s = steps[taken[0]]
            for kc in range(1, C):
                for dg in range(G if direct(m, s) else 1):
                    x_copy(m, kc, s, dg).wait_recv()
                for dg in range(1, 1 if direct(m, s) else G):
                    y_copy(m, kc, s, dg).start()
                for dg in range(G if direct(m, s) else 1):
                    p_copy(m, kc, s, dg).start()
            taken[0] += 1

    def weight_part(m, rows, cols):
        return (win, wout)[m].at[pl.ds(0, rows), pl.ds(0, cols)]

    def collect(n):
        w = weight_part(1, F, (C - 1) * De // nk) if n else weight_part(0, (C - 1) * De, F)
        remote(w, w, wp_s.at[0], wp_r.at[n], ee=partner).wait_recv()

    issue(EARLY)
    for copy in small:
        copy.wait()

    nrow = min(64, T)

    def norm_step(i, carry):
        rows = pl.ds(pl.multiple_of(i * nrow, nrow), nrow)
        x = tok[rows, :].astype(f32)
        ms = jnp.mean(x * x, axis=-1, keepdims=True)
        normed[rows, :] = (x * lax.rsqrt(ms + 1e-06) * gain[...]).astype(bf16)
        return carry

    for k in range(chunks):
        loads[k].wait()
        if k == chunks - 1:
            for copy in locals_[1:]:
                copy.start()
        lax.fori_loop(k * (T // nrow) // chunks, (k + 1) * (T // nrow) // chunks, norm_step, 0)

    picked = route[...]
    lanes = -(-E // 8) * 8
    one_hot = (lax.broadcasted_iota(jnp.int32, (lanes, T), 0) == picked).astype(f32)
    earlier = (lax.broadcasted_iota(jnp.int32, (T, T), 0) < lax.broadcasted_iota(jnp.int32, (T, T), 1))
    before = jnp.dot(one_hot.astype(bf16), earlier.astype(f32).astype(bf16), preferred_element_type=f32)
    position = jnp.sum(before * one_hot, axis=0, keepdims=True)
    slot_row = picked.astype(f32) * float(cap) + position

    def slice_at(s):
        return pl.ds(pl.multiple_of(s * share, share), share)

    def picks(q):
        dest = expert_at(q // 2, q % 2)
        wanted = slot_row - (dest * cap).astype(f32)
        return (lax.broadcasted_iota(jnp.int32, (cap, T), 0).astype(f32) == wanted).astype(f32).astype(bf16)

    def fill_slice(q, x, s):
        disp[x, (q - 2) * cap:(q - 1) * cap, :] = jnp.dot(
            picks(q), normed[:, slice_at(s)], preferred_element_type=f32).astype(bf16)

    def fill(q, dst):
        pick = picks(q)
        dn = min(512, D)

        def step(i, carry):
            cols = pl.ds(pl.multiple_of(i * dn, dn), dn)
            dst[0:cap, cols] = jnp.dot(pick, normed[:, cols], preferred_element_type=f32).astype(bf16)
            return carry

        lax.fori_loop(0, D // dn, step, 0)

    ends = ((0, Z - 1), (Z - 1, 0))

    def dx_copy(q, x, s):
        return remote(disp.at[x, pl.ds((q - 2) * cap, cap), :], arrived.at[pl.ds(q * cap, cap), slice_at(s)],
                      dx_s.at[q - 2, x], dx_r.at[q - 2, x], ee=expert_at(q // 2, q % 2))

    d1_copy = remote(dispq, arrived.at[pl.ds(cap, cap), :], d1_s.at[0], d1_r.at[0], ee=partner)

    pending = None
    for q in units:
        fill_slice(q, 0, z)
        if pending is not None:
            dx_copy(pending, 0, z).start()
        pending = q
    for at, s in ends:
        @when(z == at)
        def _():
            for q in fast:
                fill_slice(q, 1, s)
    if pending is not None:
        dx_copy(pending, 0, z).start()
    fill(1, dispq)
    for at, s in ends:
        @when(z == at)
        def _():
            for q in fast:
                dx_copy(q, 1, s).start()
    issue(len(steps))
    fill(0, arrived)
    d1_copy.start()
    for copy in own_copies:
        copy.start()

    def hop(q, way, t, s):
        part = arrived.at[pl.ds(q * cap, cap), slice_at(s)]
        return remote(part, part, ag_s.at[q - 2, way, t - 1], ag_r.at[q - 2, way, t - 1], zz=below if way else above)

    def hops(q):
        return Z - 2 if q in fast else Z - 1

    def gather(q, t, middle=True, edges=True):
        if t == 0:
            dx_copy(q, 0, z).wait_recv()
        inner = (z > 0) & (z < Z - 1)
        here = True if middle and edges else inner if middle else ~inner

        @when((z >= t) & here)
        def _():
            if t > 0:
                hop(q, 0, t, z - t).wait_recv()
        if t < hops(q) and middle:
            @when((z >= t) & (z < Z - 1))
            def _():
                hop(q, 0, t + 1, z - t).start()

        @when((z + t <= Z - 1) & here)
        def _():
            if t > 0:
                hop(q, 1, t, z + t).wait_recv()
        if t < hops(q) and middle:
            @when((z + t <= Z - 1) & (z > 0))
            def _():
                hop(q, 1, t + 1, z + t).start()

    def hidden(load, rows, w, lo=0, hi=None, at=0):
        def step(i, carry):
            cols = pl.ds(pl.multiple_of(i * 256, 256), 256)
            acc = jnp.dot(load(), w[:, cols], preferred_element_type=f32)
            hbuf[at:at + rows, cols] = jax.nn.gelu(acc).astype(bf16)
            return carry

        lax.fori_loop(lo, F // 256 if hi is None else hi, step, 0)

    blocks = F // 256

    def part_of(i, n):
        return i * blocks // n, (i + 1) * blocks // n

    pair = 2 * cap
    take(EARLY)
    first_row = lax.broadcasted_iota(jnp.int32, (128, T), 0) == 0
    turned[...] = jnp.transpose(jnp.where(first_row, slot_row, gate[...]))
    slot_col = turned[:, 0:1]
    col = lax.broadcasted_iota(jnp.int32, (T, pair), 1).astype(f32)
    here = slot_col - (e * cap).astype(f32)
    there = slot_col - (partner * cap).astype(f32) + float(cap)
    pk[...] = (((col == here) & (col < cap)) | ((col == there) & (col >= cap))).astype(f32).astype(bf16)

    locals_[1].wait()
    d1_copy.wait_recv()
    for i in range(4):
        hidden(lambda: arrived[0:pair, :], pair, ein, *part_of(i, 4))
        if i == 1:
            for q in units:
                gather(q, 0)

    locals_[2].wait()

    def own_step(i, carry):
        cols = pl.ds(pl.multiple_of(i * 256, 256), 256)
        acc = jnp.dot(hbuf[0:pair, :], eout[:, cols], preferred_element_type=f32).astype(bf16)
        pown[0:cap, cols] = acc[0:cap, :]
        psend[:, cols] = acc[cap:pair, :]
        return carry

    own_blocks = D // 256
    lax.fori_loop(0, own_blocks // 2, own_step, 0)
    if Z > 2:
        for q in units:
            gather(q, 1)
    relay(EARLY)
    lax.fori_loop(own_blocks // 2, own_blocks, own_step, 0)

    @when(z == 0)
    def _():
        rpo[0] = jnp.zeros(rpo.shape[1:], bf16)
        rpd[0] = jnp.zeros(rpd.shape[1:], bf16)

    @when(z == Z - 1)
    def _():
        rpo[Z] = jnp.zeros(rpo.shape[1:], bf16)
        rpd[Z] = jnp.zeros(rpd.shape[1:], bf16)

    pq_copy = remote(psend, pown.at[pl.ds(cap, cap), :], pq_s.at[0], pq_r.at[0], ee=partner)
    pq_copy.start()

    def zo_copy(q, d, slot, to):
        rows = pl.ds((q - 2) * cap, cap)
        return remote(po.at[d, rows, :], rpo.at[slot, rows, :], zo_s.at[0], zo_r.at[q - 2, slot], zz=to)

    def back_slot(d, to):
        return Z if d == to else d

    def zo_edge(q, i):
        @when(z == 0)
        def _():
            zo_copy(q, Z - 1 - i, Z - 1 - i, 1).start()

        @when(z == Z - 1)
        def _():
            zo_copy(q, i, back_slot(i, Z - 2), Z - 2).start()

    def expert_hidden(q, between=None):
        if q in fast:
            for at, s in ends:
                @when(z == at)
                def _():
                    dx_copy(q, 1, s).wait_recv()
        rows = slice(q * cap, (q + 1) * cap)
        hidden(lambda: arrived[rows, :], cap, ein, *part_of(0, 2))
        if between is not None:
            between()
        hidden(lambda: arrived[rows, :], cap, ein, *part_of(1, 2))

    def expert_out(q, between=None):
        rows = slice((q - 2) * cap, (q - 1) * cap)
        for i in range(Z):
            d = (1 - upper) * (Z - 1 - i) + upper * i

            def step(k, carry):
                acc = jnp.dot(hbuf[0:cap, :], eout[:, pl.ds(pl.multiple_of(d * share + k * 256, 256), 256)],
                              preferred_element_type=f32)
                po[d, rows, pl.ds(pl.multiple_of(k * 256, 256), 256)] = acc.astype(bf16)
                return carry

            lax.fori_loop(0, share // 256, step, 0)
            if i < Z - 1:
                zo_edge(q, i)
            if between is not None:
                between(i)

    def zo_up(q, d):
        @when((z > 0) & (z < d))
        def _():
            rows = slice((q - 2) * cap, (q - 1) * cap)
            zo_copy(q, d, d, above).wait_recv()
            po[d, rows, :] = (po[d, rows, :].astype(f32) + rpo[d, rows, :].astype(f32)).astype(bf16)
            zo_copy(q, d, d, above).start()

    def zo_down(q, d):
        @when((z < Z - 1) & (z > d))
        def _():
            rows = slice((q - 2) * cap, (q - 1) * cap)
            zo_copy(q, d, d, below).wait_recv()
            po[d, rows, :] = (po[d, rows, :].astype(f32) + rpo[d, rows, :].astype(f32)).astype(bf16)

        for slot, near in ((d, z > d + 1), (Z, z == d + 1)):
            @when((z < Z - 1) & near)
            def _():
                zo_copy(q, d, slot, below).start()

    def zo_near(q, t):
        @when(upper == 0)
        def _():
            zo_up(q, Z - 1 - t)

        @when(upper == 1)
        def _():
            zo_down(q, t)

    def zo_far(q, t):
        @when(upper == 0)
        def _():
            zo_down(q, t)

        @when(upper == 1)
        def _():
            zo_up(q, Z - 1 - t)

    def ret_copy(q):
        rows = pl.ds((q - 2) * cap, cap)
        return remote(ret.at[rows, :], rret.at[rows, :], ret_s.at[q - 2], ret_r.at[q - 2], ee=expert_at(-(q // 2), q % 2))

    def zo_final(q):
        @when(z > 0)
        def _():
            zo_copy(q, z, z, above).wait_recv()

        @when(z < Z - 1)
        def _():
            zo_copy(q, z, Z, above).wait_recv()
        rows = slice((q - 2) * cap, (q - 1) * cap)
        ret[rows, :] = (po[z, rows, :].astype(f32) + rpo[z, rows, :].astype(f32)
                        + rpo[Z, rows, :].astype(f32)).astype(bf16)

    def point(n):
        return n * SUBS[0] // 8 if n <= 8 else SUBS[0] + (n - 8) * SUBS[1] // 8

    def weights(to_take, to_relay):
        take(point(to_take))
        relay(point(to_relay))

    def passes(kind, group, t):
        if t < Z - 1:
            for q in group:
                kind(q, t)

    for t in range(2, Z - 1):
        for q in fast:
            gather(q, t)
    take(point(2))
    for n, q in enumerate(fast):
        final = n == len(fast) - 1
        expert_hidden(q, (lambda: take(point(3))) if final else None)
        if final:
            for k in slow:
                for t in range(2, Z - 1):
                    gather(k, t, edges=t == 0)
        expert_out(q, (lambda i: take(point(4))) if final else None)
    weights(5, 2)
    pq_copy.wait_recv()

    def own_rows(i, carry):
        cols = pl.ds(pl.multiple_of(i * 256, 256), 256)
        res = jnp.dot(pk[...], pown[:, cols], preferred_element_type=f32)
        eres[:, cols] = (turned[:, 1:2] * res).astype(bf16)
        return carry

    lax.fori_loop(0, own_blocks, own_rows, 0)

    def serve(i):
        if i == 0:
            take(point(8))
        if i == Z // 2 - 1:
            relay(point(5))
            passes(zo_near, fast, 0)
        if i == Z // 2:
            relay(point(6))

    for n, q in enumerate(slow):
        final = n == len(slow) - 1
        for t in range(2, Z - 1):
            gather(q, t, middle=False)
        gather(q, Z - 1)
        if n == 0:
            weights(6, 3)
        expert_hidden(q, (lambda: weights(7, 4)) if final else None)
        expert_out(q, serve if final else None)
    passes(zo_near, fast, 1)
    relay(point(7))
    passes(zo_far, fast, 0)
    relay(point(8))
    take(point(10))
    locals_[3].wait()
    own_copies[0].wait_recv()
    collect(0)

    nr = 2 if T % 32 == 0 else 1
    tall = T // nr
    halves = range(nr)

    def zd_copy(d, slot, c, r, to):
        rows, cols = pl.ds(r * tall, tall), pl.ds(c * wide, wide)
        n = c * nr + r
        return remote(pd.at[d, rows, cols], rpd.at[slot, rows, cols], zd_s.at[0], zd_r.at[slot, n], zz=to)

    mine = Z // C if Z % C == 0 else 0
    lined = C == 2 and nk == 2 and mine > 1
    turn = lax.rem(upper + chip, 2)

    def slice_number(i):
        if C == 2 and Z % 2 == 0:
            low = i if i < mine else Z - 1 - (i - mine)
            return chip * (Z - 1 - low) + (1 - chip) * low
        return lax.rem(chip * mine + i, Z)

    def late(i, c, r):
        return c == nk - 1 and r == nr - 1 and lined and i < mine

    def dense(i, c, group=None):
        group = halves if group is None else group
        d = slice_number(i)
        rows = slice(group[0] * tall, (group[-1] + 1) * tall)
        if lined and i < mine:
            d = turn * d + (1 - turn) * slice_number(mine - 1 - i)

        def step(k, carry):
            cols = pl.ds(pl.multiple_of(d * share + c * wide + k * tn, tn), tn)
            acc = jnp.dot(hbuf[rows, :], wout[:, cols], preferred_element_type=f32)
            pd[d, rows, pl.ds(pl.multiple_of(c * wide + k * tn, tn), tn)] = (acc + eres[rows, cols].astype(f32)).astype(bf16)
            return carry

        lax.fori_loop(0, wide // tn, step, 0)

        for r in group:
            dense_edge(i, c, r, False, d)

    def dense_edge(i, c, r, again, d):
        beside = ((z == 0) & (d == 1)) | ((z == Z - 1) & (d == Z - 2))
        go = (beside if again else ~beside) if late(i, c, r) else True
        if again and not late(i, c, r):
            return

        @when((z == 0) & (d > 0) & go)
        def _():
            zd_copy(d, d, c, r, above).start()

        for slot, near in ((d, z > d + 1), (Z, z == d + 1)):
            @when((z == Z - 1) & near & go)
            def _():
                zd_copy(d, slot, c, r, below).start()

    def zd_pass(i, c, r):
        d = slice_number(i)
        rows, cols = pl.ds(r * tall, tall), pl.ds(c * wide, wide)

        @when((z > 0) & (z < Z - 1) & (z != d))
        def _():
            zd_copy(d, d, c, r, above).wait_recv()
            pd[d, rows, cols] = (pd[d, rows, cols].astype(f32) + rpd[d, rows, cols].astype(f32)).astype(bf16)

        @when((z > 0) & (z < d))
        def _():
            zd_copy(d, d, c, r, above).start()

        for slot, near in ((d, z > d + 1), (Z, z == d + 1)):
            @when((z < Z - 1) & near)
            def _():
                zd_copy(d, slot, c, r, below).start()

    trow = min(128, T)
    residual = slice_at(z)

    def combine_experts():
        for q in units:
            ret_copy(q).wait_recv()
        for i in range(T // trow):
            rows = slice(i * trow, (i + 1) * trow)
            res = jnp.zeros((trow, share), f32)
            for q in units:
                wanted = turned[rows, 0:1] - (expert_at(q // 2, q % 2) * cap).astype(f32)
                pick = (lax.broadcasted_iota(jnp.int32, (trow, cap), 1).astype(f32) == wanted)
                res = res + jnp.dot(pick.astype(f32).astype(bf16), rret[(q - 2) * cap:(q - 1) * cap, :],
                                    preferred_element_type=f32)
            base[rows, :] = tok[rows, residual].astype(f32) + turned[rows, 1:2] * res

    def sent():
        for copy in own_copies:
            copy.wait_send()
        d1_copy.wait_send()
        pq_copy.wait_send()
        for q in units:
            dx_copy(q, 0, z).wait_send()
            ret_copy(q).wait_send()
            for at, s in ends:
                @when((z == at) & (q in fast))
                def _():
                    dx_copy(q, 1, s).wait_send()
            for t in range(1, hops(q) + 1):
                @when((z >= t - 1) & (z < Z - 1))
                def _():
                    hop(q, 0, t, z - t + 1).wait_send()

                @when((z + t - 1 <= Z - 1) & (z > 0))
                def _():
                    hop(q, 1, t, z + t - 1).wait_send()
        for m in range(2):
            for sem, n in ((wx_s, 1), (wy_s, G - 1), (wp_s, G)):
                rows, cols = ((C - 1) * De // G * n, F) if m == 0 else (F // G * n, (C - 1) * De)
                if direct(m, SUBS[0] - 1) and sem is not wp_s:
                    extra = (C - 1) * (G - 1) * De // G // SUBS[0]
                    rows += extra if sem is wx_s else -extra
                w = weight_part(m, rows, cols)
                remote(w, w, sem.at[m], wp_r.at[0], ee=partner).wait_send()

    def finish(c):
        cols = slice(c * wide, (c + 1) * wide)

        for r in halves:
            @when(z > 0)
            def _():
                zd_copy(z, z, c, r, above).wait_recv()

            @when(z < Z - 1)
            def _():
                zd_copy(z, Z, c, r, above).wait_recv()

        for i in range(T // trow):
            rows = slice(i * trow, (i + 1) * trow)
            total = pd[z, rows, cols].astype(f32) + rpd[z, rows, cols].astype(f32) + rpd[Z, rows, cols].astype(f32)
            out[rows, cols] = (base[rows, cols] + total).astype(bf16)

    per = SUBS[1] // nk
    def along(kind):
        for i, c, r in kind:
            zd_pass(i, c, r)

    def in_turn(first_kind, second_kind):
        if not lined:
            return

        @when(turn == 0)
        def _():
            along(first_kind)

        @when(turn == 1)
        def _():
            along(second_kind)

    near, far = list(range(mine, Z)), list(range(mine))
    n0, n1, f0 = near[0], near[1:], far[0] if far else 0

    def both(items, c):
        return [(i, c, r) for i in items for r in halves]

    def rest_of(items, c):
        return [(i, c, r) for i in items for r in halves[1:]]


    def mlp_hidden(group, i, n):
        rows = slice(group[0] * tall, (group[-1] + 1) * tall)
        hidden(lambda: normed[rows, :], len(group) * tall, win, *part_of(i, n), at=group[0] * tall)

    groups = [halves[:1], halves[1:]] if lined else [halves]
    mlp_hidden(groups[0], 0, 2)
    weights(11, 9)
    mlp_hidden(groups[0], 1, 2)
    locals_[4].wait()
    own_copies[1].wait_recv()
    if lined:
        dense(0, 0, groups[0])
        dense(0, 1, groups[0])
    take(point(12))
    passes(zo_far, fast, 1)
    for t in range(2, Z - 1):
        passes(zo_near, fast, t)
        passes(zo_far, fast, t)
    relay(point(10))
    if lined:
        mlp_hidden(groups[1], 0, 2)
        passes(zo_near, slow, 0)
        mlp_hidden(groups[1], 1, 2)
        weights(13, 11)
        dense(0, 0, groups[1])
        dense(1, 0)
    else:
        passes(zo_near, slow, 0)
        weights(13, 11)
        for i in range(mine):
            dense(i, 0)
    weights(14, 12)
    passes(zo_near, slow, 1)
    passes(zo_far, slow, 0)
    in_turn([], [(f0, 0, 0)])
    if nk > 1:
        collect(1)
        for i in range(mine, Z):
            dense(i, 0)
        weights(15, 13)
        passes(zo_far, slow, 1)
        for q in fast:
            zo_final(q)
            ret_copy(q).start()
        in_turn([(n0, 0, 0)], [(f0, 1, 0)] + rest_of([f0], 0))
        for c in range(1, nk):
            for i in range(mine):
                dense(i, c, groups[-1] if i == 0 else halves)
    weights(16, 14)
    for t in range(1 if nk == 1 else 2, Z - 1):
        passes(zo_near, slow, t)
        passes(zo_far, slow, t)
    for q in slow if nk > 1 else units:
        zo_final(q)
        ret_copy(q).start()
    in_turn(rest_of([n0], 0), both(far[1:], 0))
    relay(point(15))
    in_turn([(i, 0, 0) for i in n1[:1]], [(n0, 0, 0)])
    relay(point(16))
    collect(nk)
    for i in range(mine, Z):
        dense(i, nk - 1)
        if i == mine:
            in_turn(rest_of(n1[:1], 0), rest_of([n0], 0))
    for c in range(nk):
        for i in range(Z):
            for r in halves:
                dense_edge(i, c, r, True, slice_number(i))
    in_turn(both(far, 0) + both(n1[1:], 0), both(n1, 0))
    if not lined:
        along([(i, 0, r) for i in range(Z) for r in halves])
    combine_experts()
    in_turn([(f0, 1, 0), (n0, 1, 0)], rest_of([f0], 1))
    sent()
    in_turn(rest_of([n0], 1) + rest_of([f0], 1) + both(far[1:], 1) + both(n1, 1),
            both(far[1:], 1) + both(near, 1))
    if not lined:
        along([(i, c, r) for c in range(1, nk) for i in range(Z) for r in halves])
    for c in range(nk):
        finish(c)

    def last_waits():
        for array, sem in ((po, zo_s), (pd, zd_s)):
            part = array.at[pl.ds(0, Z - 1)]
            remote(part, part, sem.at[0], wp_r.at[0], ee=partner).wait_send()

    last_waits()


def local(tokens, route, gate_prob, norm_gain, dense_in, dense_out, expert_in, expert_out):
    G, E, Z = lax.axis_size("groups"), lax.axis_size("expert"), lax.axis_size("cuts")
    T, D = tokens.shape
    F = dense_in.shape[1]
    share = D // Z
    De = D // E
    cap = max(2, 3 * T // (2 * E))
    C = E // 2
    away = E - 2
    others = away * cap
    nk = 2 if De == share and share % 256 == 0 else 1
    bf16 = jnp.bfloat16
    any_, vmem = pl.BlockSpec(memory_space=pl.ANY), pl.BlockSpec(memory_space=pltpu.VMEM)
    dma = pltpu.SemaphoreType.DMA
    splits = (max(1, min(8, De // (16 * G))), 8)
    subs = max(splits)
    return pl.pallas_call(
        functools.partial(kernel, G, E, Z, cap, nk, splits),
        out_shape=jax.ShapeDtypeStruct((T, share), bf16),
        in_specs=[any_, any_, any_, any_, any_, any_, any_, any_],
        out_specs=vmem,
        scratch_shapes=[
            pltpu.VMEM((D, F), bf16), pltpu.VMEM((F, D), bf16),
            pltpu.VMEM((D, F), bf16), pltpu.VMEM((F, D), bf16),
            pltpu.VMEM((T, D), bf16), pltpu.VMEM((T, D), bf16),
            pltpu.VMEM((2, others, share), bf16), pltpu.VMEM((cap, D), bf16), pltpu.VMEM((E * cap, D), bf16),
            pltpu.VMEM((max(T, 2 * cap), F), bf16),
            pltpu.VMEM((2 * cap, D), bf16), pltpu.VMEM((cap, D), bf16),
            pltpu.VMEM((Z, others, share), bf16), pltpu.VMEM((Z + 1, others, share), bf16),
            pltpu.VMEM((Z, T, share), bf16), pltpu.VMEM((Z + 1, T, share), bf16),
            pltpu.VMEM((others, share), bf16), pltpu.VMEM((others, share), bf16),
            pltpu.VMEM((T, share), jnp.float32), pltpu.VMEM((T, 2 * cap), bf16),
            pltpu.VMEM((T, 128), jnp.float32), pltpu.VMEM((T, D), bf16),
            pltpu.VMEM((1, T), jnp.int32), pltpu.VMEM((1, T), jnp.float32), pltpu.VMEM((1, D), jnp.float32),
            dma((12,)), dma((2,)), dma((2,)), dma((1,)), dma((1,)), dma((away, 2)), dma((away, 2)),
            dma((away, 2, Z - 1)), dma((away, 2, Z - 1)), dma((1,)), dma((1,)),
            dma((2,)), dma((2, C - 1, subs + G - 1)), dma((2,)), dma((2, C - 1, subs, G - 1)), dma((2,)), dma((1 + nk,)),
            dma((1,)), dma((away, Z + 1)), dma((1,)), dma((Z + 1, 2 * nk)), dma((away,)), dma((away,)),
        ],
        compiler_params=pltpu.CompilerParams(
            collective_id=0, has_side_effects=True, vmem_limit_bytes=67043328
        ),
    )(tokens, route.reshape(1, T), gate_prob[None, :], norm_gain[None, :], dense_in, dense_out, expert_in, expert_out)


def solution(mesh):
    return jax.shard_map(
        local,
        mesh=mesh,
        in_specs=(
            P(("groups", "expert"), None),
            P(("groups", "expert"), None),
            P(("groups", "expert")),
            P(),
            P("expert", "cuts"),
            P("cuts", "expert"),
            P("expert", None, "cuts"),
            P("expert", "cuts", None),
        ),
        out_specs=P(("groups", "expert"), "cuts"),
        check_vma=False,
    )
```

```python
import functools

import jax
import jax.numpy as jnp
from jax import lax
from jax.experimental import pallas as pl
from jax.experimental.pallas import tpu as pltpu
from jax.sharding import PartitionSpec as P


def kernel(G, E, Z, cap, nk, SUBS, tokens, route_h, gate_h, gain_h, din, dout, ein_h, eout_h, out,
           win, wout, ein, eout, tok, normed, disp, dispq, arrived, hbuf, pown, psend, po, rpo, pd, rpd,
           ret, rret, base, pk, turned, eres, acc, route, gate, gain,
           loc, own_s, own_r, d1_s, d1_r, dx_s, dx_r, ag_s, ag_r, pq_s, pq_r,
           wx_s, wx_r, wy_s, wy_r, wp_s, wp_r, zo_s, zo_r, zd_s, zd_r, ret_s, ret_r):
    f32, bf16 = jnp.float32, jnp.bfloat16
    T, D = tok.shape
    F = ein.shape[1]
    De = D // E
    share = D // Z
    C = E // 2
    wide = share // nk
    tn = min(256, wide)
    units = range(2, E)
    fast, slow = units[:(E - 2) // 2], units[(E - 2) // 2:]
    g, e, z = lax.axis_index("groups"), lax.axis_index("expert"), lax.axis_index("cuts")
    chip, core = e // 2, lax.rem(e, 2)
    partner = chip * 2 + 1 - core
    above, below = lax.rem(z + 1, Z), lax.rem(z + Z - 1, Z)
    upper = (2 * z) // Z

    def remote(src, dst, send, recv, gg=None, ee=None, zz=None):
        return pltpu.make_async_remote_copy(
            src_ref=src, dst_ref=dst, send_sem=send, recv_sem=recv,
            device_id={
                "groups": g if gg is None else gg,
                "expert": e if ee is None else ee,
                "cuts": z if zz is None else zz,
            },
            device_id_type=pl.DeviceIdType.MESH,
        )

    def when(condition):
        return pl.when(condition)

    def expert_at(kc, j):
        other = lax.rem(chip + kc + C, C)
        return other * 2 + (core if j == 0 else 1 - core)

    my_rows = pl.ds(pl.multiple_of(e * De, De), De)
    locals_ = [
        pltpu.make_async_copy(route_h, route, loc.at[0]),
        pltpu.make_async_copy(ein_h.at[0], ein, loc.at[1]),
        pltpu.make_async_copy(eout_h.at[0], eout, loc.at[2]),
        pltpu.make_async_copy(din, win.at[my_rows, :], loc.at[3]),
        pltpu.make_async_copy(dout, wout.at[:, my_rows], loc.at[4]),
    ]
    chunks = 4 if T % 256 == 0 else 1
    loads = []
    for k in range(chunks):
        part = pl.ds(k * (T // chunks), T // chunks)
        loads.append(pltpu.make_async_copy(tokens.at[part, :], tok.at[part, :], loc.at[5 + k]))
    small = [
        pltpu.make_async_copy(gain_h, gain, loc.at[9]),
        pltpu.make_async_copy(gate_h, gate, loc.at[10]),
        locals_[0],
    ]
    for copy in small + loads:
        copy.start()

    barrier = pltpu.get_barrier_semaphore()
    for k in range(1, E):
        pl.semaphore_signal(barrier, inc=1, device_id={"groups": g, "expert": lax.rem(e + k, E), "cuts": z},
                            device_id_type=pl.DeviceIdType.MESH)
    for k in range(1, Z):
        pl.semaphore_signal(barrier, inc=1, device_id={"groups": g, "expert": e, "cuts": lax.rem(z + k, Z)},
                            device_id_type=pl.DeviceIdType.MESH)
    for k in range(1, G):
        pl.semaphore_signal(barrier, inc=1, device_id={"groups": lax.rem(g + k, G), "expert": e, "cuts": z},
                            device_id_type=pl.DeviceIdType.MESH)

    own_copies = [
        remote(din, win.at[my_rows, :], own_s.at[0], own_r.at[0], ee=partner),
        remote(dout, wout.at[:, my_rows], own_s.at[1], own_r.at[1], ee=partner),
    ]

    def block(m, p, s):
        if m == 0:
            n = De // G // SUBS[0]
            return p * (De // G) + s * n, n, 0, F
        per = SUBS[1] // nk
        n = F // G // per
        return p * (F // G) + (s % per) * n, n, (s // per) * (De // nk), De // nk

    def weight(m, owner, p, s):
        row, n, col, width = block(m, p, s)
        if m == 0:
            return win.at[pl.ds(pl.multiple_of(owner * De + row, n), n), :]
        return wout.at[pl.ds(pl.multiple_of(row, n), n),
                       pl.ds(pl.multiple_of(owner * De + col, width), width)]

    def weight_source(m, p, s):
        row, n, col, width = block(m, p, s)
        return (din, dout)[m].at[pl.ds(pl.multiple_of(row, n), n), pl.ds(col, width)]

    def direct(m, s):
        per = SUBS[0] if m == 0 else SUBS[1] // nk
        return per > 1 and s % per == per - 1

    def x_copy(m, kc, s, dg=0):
        half = lax.rem(g - dg + G, G)
        group = s // (SUBS[1] // nk) if m else 0
        place = s if dg == 0 else max(SUBS) + group * (G - 1) + dg - 1
        return remote(weight_source(m, half, s), weight(m, e, half, s), wx_s.at[m],
                      wx_r.at[m, kc - 1, place], ee=expert_at(kc, 0))

    def y_copy(m, kc, s, dg):
        w = weight(m, expert_at(-kc, 0), g, s)
        return remote(w, w, wy_s.at[m], wy_r.at[m, kc - 1, s, dg - 1], gg=lax.rem(g + dg, G))

    def p_copy(m, kc, s, dg):
        w = weight(m, expert_at(-kc, 0), lax.rem(g - dg + G, G), s)
        return remote(w, w, wp_s.at[m], wp_r.at[m * (1 + s // (SUBS[1] // nk))], ee=partner)

    steps = [(m, s) for m in range(2) for s in range(SUBS[m])]
    issued, taken, relayed = [0], [0], [0]

    def issue(upto):
        while issued[0] < min(upto, len(steps)):
            m, s = steps[issued[0]]
            for kc in range(1, C):
                for dg in range(G if direct(m, s) else 1):
                    x_copy(m, kc, s, dg).start()
            issued[0] += 1

    def relay(upto):
        while relayed[0] < min(upto, taken[0]):
            m, s = steps[relayed[0]]
            for kc in range(1, C):
                for dg in range(1, 1 if direct(m, s) else G):
                    y_copy(m, kc, s, dg).wait_recv()
                    p_copy(m, kc, s, dg).start()
            relayed[0] += 1

    def take(upto):
        while taken[0] < min(upto, len(steps)):
            m, s = steps[taken[0]]
            for kc in range(1, C):
                for dg in range(G if direct(m, s) else 1):
                    x_copy(m, kc, s, dg).wait_recv()
                for dg in range(1, 1 if direct(m, s) else G):
                    y_copy(m, kc, s, dg).start()
                for dg in range(G if direct(m, s) else 1):
                    p_copy(m, kc, s, dg).start()
            taken[0] += 1

    def weight_part(m, rows, cols):
        return (win, wout)[m].at[pl.ds(0, rows), pl.ds(0, cols)]

    def collect(n):
        w = weight_part(1, F, (C - 1) * De // nk) if n else weight_part(0, (C - 1) * De, F)
        remote(w, w, wp_s.at[0], wp_r.at[n], ee=partner).wait_recv()

    for copy in small:
        copy.wait()

    nrow = min(64, T)

    def norm_step(i, carry):
        rows = pl.ds(pl.multiple_of(i * nrow, nrow), nrow)
        x = tok[rows, :].astype(f32)
        ms = jnp.mean(x * x, axis=-1, keepdims=True)
        normed[rows, :] = (x * lax.rsqrt(ms + 1e-06) * gain[...]).astype(bf16)
        return carry

    for k in range(chunks):
        loads[k].wait()
        if k == chunks - 1:
            for copy in locals_[1:]:
                copy.start()
        lax.fori_loop(k * (T // nrow) // chunks, (k + 1) * (T // nrow) // chunks, norm_step, 0)

    picked = route[...]
    lanes = -(-E // 8) * 8
    one_hot = (lax.broadcasted_iota(jnp.int32, (lanes, T), 0) == picked).astype(f32)
    earlier = (lax.broadcasted_iota(jnp.int32, (T, T), 0) < lax.broadcasted_iota(jnp.int32, (T, T), 1))
    before = jnp.dot(one_hot.astype(bf16), earlier.astype(f32).astype(bf16), preferred_element_type=f32)
    position = jnp.sum(before * one_hot, axis=0, keepdims=True)
    slot_row = picked.astype(f32) * float(cap) + position

    def slice_at(s):
        return pl.ds(pl.multiple_of(s * share, share), share)

    def picks(q):
        dest = expert_at(q // 2, q % 2)
        wanted = slot_row - (dest * cap).astype(f32)
        return (lax.broadcasted_iota(jnp.int32, (cap, T), 0).astype(f32) == wanted).astype(f32).astype(bf16)

    def fill_slice(q, x, s):
        disp[x, (q - 2) * cap:(q - 1) * cap, :] = jnp.dot(
            picks(q), normed[:, slice_at(s)], preferred_element_type=f32).astype(bf16)

    def fill(q, dst):
        pick = picks(q)
        dn = min(512, D)

        def step(i, carry):
            cols = pl.ds(pl.multiple_of(i * dn, dn), dn)
            dst[0:cap, cols] = jnp.dot(pick, normed[:, cols], preferred_element_type=f32).astype(bf16)
            return carry

        lax.fori_loop(0, D // dn, step, 0)

    ends = ((0, Z - 1), (Z - 1, 0))

    def dx_copy(q, x, s):
        return remote(disp.at[x, pl.ds((q - 2) * cap, cap), :], arrived.at[pl.ds(q * cap, cap), slice_at(s)],
                      dx_s.at[q - 2, x], dx_r.at[q - 2, x], ee=expert_at(q // 2, q % 2))

    d1_copy = remote(dispq, arrived.at[pl.ds(cap, cap), :], d1_s.at[0], d1_r.at[0], ee=partner)

    for q in units:
        fill_slice(q, 0, z)
    pl.semaphore_wait(barrier, (E - 1) + (Z - 1) + (G - 1))
    for q in units:
        dx_copy(q, 0, z).start()
    for at, s in ends:
        @when(z == at)
        def _():
            for q in fast:
                fill_slice(q, 1, s)
    fill(1, dispq)
    for at, s in ends:
        @when(z == at)
        def _():
            for q in fast:
                dx_copy(q, 1, s).start()
    issue(len(steps))
    fill(0, arrived)
    d1_copy.start()
    for copy in own_copies:
        copy.start()

    def hop(q, way, t, s):
        part = arrived.at[pl.ds(q * cap, cap), slice_at(s)]
        return remote(part, part, ag_s.at[q - 2, way, t - 1], ag_r.at[q - 2, way, t - 1], zz=below if way else above)

    def hops(q):
        return Z - 2 if q in fast else Z - 1

    def gather(q, t, middle=True, edges=True):
        if t == 0:
            dx_copy(q, 0, z).wait_recv()
        inner = (z > 0) & (z < Z - 1)
        here = True if middle and edges else inner if middle else ~inner

        @when((z >= t) & here)
        def _():
            if t > 0:
                hop(q, 0, t, z - t).wait_recv()
        if t < hops(q) and middle:
            @when((z >= t) & (z < Z - 1))
            def _():
                hop(q, 0, t + 1, z - t).start()

        @when((z + t <= Z - 1) & here)
        def _():
            if t > 0:
                hop(q, 1, t, z + t).wait_recv()
        if t < hops(q) and middle:
            @when((z + t <= Z - 1) & (z > 0))
            def _():
                hop(q, 1, t + 1, z + t).start()

    def hidden(load, rows, w, lo=0, hi=None, at=0):
        def step(i, carry):
            cols = pl.ds(pl.multiple_of(i * 256, 256), 256)
            product = jnp.dot(load(), w[:, cols], preferred_element_type=f32)
            hbuf[at:at + rows, cols] = jax.nn.gelu(product).astype(bf16)
            return carry

        lax.fori_loop(lo, F // 256 if hi is None else hi, step, 0)

    blocks = F // 256

    def part_of(i, n):
        return i * blocks // n, (i + 1) * blocks // n

    pair = 2 * cap
    first_row = lax.broadcasted_iota(jnp.int32, (128, T), 0) == 0
    turned[...] = jnp.transpose(jnp.where(first_row, slot_row, gate[...]))
    slot_col = turned[:, 0:1]
    col = lax.broadcasted_iota(jnp.int32, (T, pair), 1).astype(f32)
    here = slot_col - (e * cap).astype(f32)
    there = slot_col - (partner * cap).astype(f32) + float(cap)
    pk[...] = (((col == here) & (col < cap)) | ((col == there) & (col >= cap))).astype(f32).astype(bf16)

    locals_[1].wait()
    d1_copy.wait_recv()
    for i in range(4):
        hidden(lambda: arrived[0:pair, :], pair, ein, *part_of(i, 4))
        if i == 1:
            for q in fast:
                gather(q, 0)
    for q in slow:
        gather(q, 0)

    locals_[2].wait()

    def own_step(i, carry):
        cols = pl.ds(pl.multiple_of(i * 256, 256), 256)
        acc = jnp.dot(hbuf[0:pair, :], eout[:, cols], preferred_element_type=f32).astype(bf16)
        pown[0:cap, cols] = acc[0:cap, :]
        psend[:, cols] = acc[cap:pair, :]
        return carry

    own_blocks = D // 256
    lax.fori_loop(0, own_blocks // 2, own_step, 0)

    ahead = Z == 4 and len(fast) == 1
    last_fast, last_slow = lax.rem(z + 2, Z), (Z - 1) * (1 - upper)

    def take_extra(q):
        for at, s in ends:
            @when(z == at)
            def _():
                dx_copy(q, 1, s).wait_recv()

    def slice_dot(q, s, cols):
        return jnp.dot(arrived[q * cap:(q + 1) * cap, slice_at(s)], ein[slice_at(s), cols],
                       preferred_element_type=f32)

    def multiply_ahead(q, last):
        def step(i, carry):
            cols = pl.ds(pl.multiple_of(i * 256, 256), 256)
            acc[:, cols] = sum(slice_dot(q, lax.rem(last + k, Z), cols) for k in range(1, Z))
            return carry

        lax.fori_loop(0, blocks, step, 0)

    def multiply_last(q, last, at):
        def step(i, carry):
            cols = pl.ds(pl.multiple_of(i * 256, 256), 256)
            hbuf[at:at + cap, cols] = jax.nn.gelu(acc[:, cols] + slice_dot(q, last, cols)).astype(bf16)
            return carry

        lax.fori_loop(0, blocks, step, 0)

    if Z > 2:
        for q in fast:
            gather(q, 1)
    if ahead:
        take_extra(fast[0])
        multiply_ahead(fast[0], last_fast)
    if Z > 2:
        for q in slow:
            gather(q, 1)

    def own_rest():
        lax.fori_loop(own_blocks // 2, own_blocks, own_step, 0)
        pq_copy.start()

    @when(z == 0)
    def _():
        rpo[0] = jnp.zeros(rpo.shape[1:], bf16)
        rpd[0] = jnp.zeros(rpd.shape[1:], bf16)

    @when(z == Z - 1)
    def _():
        rpo[Z] = jnp.zeros(rpo.shape[1:], bf16)
        rpd[Z] = jnp.zeros(rpd.shape[1:], bf16)

    pq_copy = remote(psend, pown.at[pl.ds(cap, cap), :], pq_s.at[0], pq_r.at[0], ee=partner)
    if not ahead:
        own_rest()

    def zo_copy(q, d, slot, to):
        rows = pl.ds((q - 2) * cap, cap)
        return remote(po.at[d, rows, :], rpo.at[slot, rows, :], zo_s.at[0], zo_r.at[q - 2, slot], zz=to)

    def back_slot(d, to):
        return Z if d == to else d

    def zo_edge(q, i):
        @when(z == 0)
        def _():
            zo_copy(q, Z - 1 - i, Z - 1 - i, 1).start()

        @when(z == Z - 1)
        def _():
            zo_copy(q, i, back_slot(i, Z - 2), Z - 2).start()

    def expert_hidden(q, between=None):
        if q in fast:
            take_extra(q)
        rows = slice(q * cap, (q + 1) * cap)
        hidden(lambda: arrived[rows, :], cap, ein, *part_of(0, 2))
        if between is not None:
            between()
        hidden(lambda: arrived[rows, :], cap, ein, *part_of(1, 2))

    def expert_out(q, between=None, at=0):
        rows = slice((q - 2) * cap, (q - 1) * cap)
        for i in range(Z):
            d = (1 - upper) * (Z - 1 - i) + upper * i

            def step(k, carry):
                acc = jnp.dot(hbuf[at:at + cap, :], eout[:, pl.ds(pl.multiple_of(d * share + k * 256, 256), 256)],
                              preferred_element_type=f32)
                po[d, rows, pl.ds(pl.multiple_of(k * 256, 256), 256)] = acc.astype(bf16)
                return carry

            lax.fori_loop(0, share // 256, step, 0)
            if i < Z - 1:
                zo_edge(q, i)
            if between is not None:
                between(i)

    def zo_up(q, d):
        @when((z > 0) & (z < d))
        def _():
            rows = slice((q - 2) * cap, (q - 1) * cap)
            zo_copy(q, d, d, above).wait_recv()
            po[d, rows, :] = (po[d, rows, :].astype(f32) + rpo[d, rows, :].astype(f32)).astype(bf16)
            zo_copy(q, d, d, above).start()

    def zo_down(q, d):
        @when((z < Z - 1) & (z > d))
        def _():
            rows = slice((q - 2) * cap, (q - 1) * cap)
            zo_copy(q, d, d, below).wait_recv()
            po[d, rows, :] = (po[d, rows, :].astype(f32) + rpo[d, rows, :].astype(f32)).astype(bf16)

        for slot, near in ((d, z > d + 1), (Z, z == d + 1)):
            @when((z < Z - 1) & near)
            def _():
                zo_copy(q, d, slot, below).start()

    def zo_near(q, t):
        @when(upper == 0)
        def _():
            zo_up(q, Z - 1 - t)

        @when(upper == 1)
        def _():
            zo_down(q, t)

    def zo_far(q, t):
        @when(upper == 0)
        def _():
            zo_down(q, t)

        @when(upper == 1)
        def _():
            zo_up(q, Z - 1 - t)

    def ret_copy(q):
        rows = pl.ds((q - 2) * cap, cap)
        return remote(ret.at[rows, :], rret.at[rows, :], ret_s.at[q - 2], ret_r.at[q - 2], ee=expert_at(-(q // 2), q % 2))

    def zo_final(q):
        @when(z > 0)
        def _():
            zo_copy(q, z, z, above).wait_recv()

        @when(z < Z - 1)
        def _():
            zo_copy(q, z, Z, above).wait_recv()
        rows = slice((q - 2) * cap, (q - 1) * cap)
        ret[rows, :] = (po[z, rows, :].astype(f32) + rpo[z, rows, :].astype(f32)
                        + rpo[Z, rows, :].astype(f32)).astype(bf16)

    def point(n):
        return n * SUBS[0] // 8 if n <= 8 else SUBS[0] + (n - 8) * SUBS[1] // 8

    def weights(to_take, to_relay):
        take(point(to_take))
        relay(point(to_relay))

    def passes(kind, group, t):
        if t < Z - 1:
            for q in group:
                kind(q, t)

    take(point(1))
    for t in range(2, Z - 1):
        for q in fast:
            gather(q, t)
    take(point(2))

    def slow_hops():
        for k in slow:
            for t in range(2, Z - 1):
                gather(k, t, edges=t == 0)

    def serve_fast(i):
        if i == 0:
            take(point(3))
        if i == 1:
            slow_hops()
        if i == Z - 1:
            take(point(4))

    if ahead:
        multiply_last(fast[0], last_fast, pair)
        expert_out(fast[0], serve_fast, pair)
        own_rest()
    else:
        for n, q in enumerate(fast):
            expert_hidden(q)
            expert_out(q, serve_fast if n == len(fast) - 1 else None)
    weights(5, 2)

    def own_rows(i, carry):
        cols = pl.ds(pl.multiple_of(i * 256, 256), 256)
        res = jnp.dot(pk[...], pown[:, cols], preferred_element_type=f32)
        eres[:, cols] = (turned[:, 1:2] * res).astype(bf16)
        return carry

    def serve_hidden():
        weights(7, 4)
        passes(zo_near, fast, 0)

    def serve(i):
        if i == Z // 2:
            relay(point(6))

    for n, q in enumerate(slow):
        final = n == len(slow) - 1
        for t in range(2, Z - 1):
            gather(q, t, middle=False)
        if ahead:
            multiply_ahead(q, last_slow)
        gather(q, Z - 1)
        if n == 0:
            weights(6, 3)
        if ahead:
            multiply_last(q, last_slow, 0)
            serve_hidden()
        else:
            expert_hidden(q, serve_hidden if final else None)
        if final:
            relay(point(5))
        expert_out(q, serve if final else None)
    passes(zo_near, fast, 1)
    take(point(8))
    pq_copy.wait_recv()
    lax.fori_loop(0, own_blocks, own_rows, 0)
    relay(point(7))
    passes(zo_far, fast, 0)
    relay(point(8))
    locals_[3].wait()
    own_copies[0].wait_recv()
    collect(0)
    take(point(9))

    nr = 2 if T % 32 == 0 else 1
    tall = T // nr
    halves = range(nr)

    def zd_copy(d, slot, c, r, to):
        rows, cols = pl.ds(r * tall, tall), pl.ds(c * wide, wide)
        n = c * nr + r
        return remote(pd.at[d, rows, cols], rpd.at[slot, rows, cols], zd_s.at[0], zd_r.at[slot, n], zz=to)

    mine = Z // C if Z % C == 0 else 0
    lined = C == 2 and nk == 2 and mine > 1
    turn = lax.rem(upper + chip, 2)

    def slice_number(i):
        if C == 2 and Z % 2 == 0:
            low = i if i < mine else Z - 1 - (i - mine)
            return chip * (Z - 1 - low) + (1 - chip) * low
        return lax.rem(chip * mine + i, Z)

    def late(i, c, r):
        return c == nk - 1 and r == nr - 1 and lined and i < mine

    def dense(i, c, group=None):
        group = halves if group is None else group
        d = slice_number(i)
        rows = slice(group[0] * tall, (group[-1] + 1) * tall)
        if lined and i < mine:
            d = turn * d + (1 - turn) * slice_number(mine - 1 - i)

        def step(k, carry):
            cols = pl.ds(pl.multiple_of(d * share + c * wide + k * tn, tn), tn)
            acc = jnp.dot(hbuf[rows, :], wout[:, cols], preferred_element_type=f32)
            pd[d, rows, pl.ds(pl.multiple_of(c * wide + k * tn, tn), tn)] = (acc + eres[rows, cols].astype(f32)).astype(bf16)
            return carry

        lax.fori_loop(0, wide // tn, step, 0)

        for r in group:
            dense_edge(i, c, r, False, d)

    def dense_edge(i, c, r, again, d):
        beside = ((z == 0) & (d == 1)) | ((z == Z - 1) & (d == Z - 2))
        go = (beside if again else ~beside) if late(i, c, r) else True
        if again and not late(i, c, r):
            return

        @when((z == 0) & (d > 0) & go)
        def _():
            zd_copy(d, d, c, r, above).start()

        for slot, near in ((d, z > d + 1), (Z, z == d + 1)):
            @when((z == Z - 1) & near & go)
            def _():
                zd_copy(d, slot, c, r, below).start()

    def zd_pass(i, c, r):
        d = slice_number(i)
        rows, cols = pl.ds(r * tall, tall), pl.ds(c * wide, wide)

        @when((z > 0) & (z < Z - 1) & (z != d))
        def _():
            zd_copy(d, d, c, r, above).wait_recv()
            pd[d, rows, cols] = (pd[d, rows, cols].astype(f32) + rpd[d, rows, cols].astype(f32)).astype(bf16)

        @when((z > 0) & (z < d))
        def _():
            zd_copy(d, d, c, r, above).start()

        for slot, near in ((d, z > d + 1), (Z, z == d + 1)):
            @when((z < Z - 1) & near)
            def _():
                zd_copy(d, slot, c, r, below).start()

    trow = min(128, T)
    residual = slice_at(z)

    def combine_experts():
        for q in units:
            ret_copy(q).wait_recv()
        for i in range(T // trow):
            rows = slice(i * trow, (i + 1) * trow)
            res = jnp.zeros((trow, share), f32)
            for q in units:
                wanted = turned[rows, 0:1] - (expert_at(q // 2, q % 2) * cap).astype(f32)
                pick = (lax.broadcasted_iota(jnp.int32, (trow, cap), 1).astype(f32) == wanted)
                res = res + jnp.dot(pick.astype(f32).astype(bf16), rret[(q - 2) * cap:(q - 1) * cap, :],
                                    preferred_element_type=f32)
            base[rows, :] = tok[rows, residual].astype(f32) + turned[rows, 1:2] * res

    def sent():
        for copy in own_copies:
            copy.wait_send()
        d1_copy.wait_send()
        pq_copy.wait_send()
        for q in units:
            dx_copy(q, 0, z).wait_send()
            ret_copy(q).wait_send()
            for at, s in ends:
                @when((z == at) & (q in fast))
                def _():
                    dx_copy(q, 1, s).wait_send()
            for t in range(1, hops(q) + 1):
                @when((z >= t - 1) & (z < Z - 1))
                def _():
                    hop(q, 0, t, z - t + 1).wait_send()

                @when((z + t - 1 <= Z - 1) & (z > 0))
                def _():
                    hop(q, 1, t, z + t - 1).wait_send()
        for m in range(2):
            for sem, n in ((wx_s, 1), (wy_s, G - 1), (wp_s, G)):
                rows, cols = ((C - 1) * De // G * n, F) if m == 0 else (F // G * n, (C - 1) * De)
                if direct(m, SUBS[m] - 1) and sem is not wp_s:
                    extra = (C - 1) * (G - 1) * De // G // SUBS[0] if m == 0 else (G - 1) * F // G // (SUBS[1] // nk)
                    rows += extra if sem is wx_s else -extra
                w = weight_part(m, rows, cols)
                remote(w, w, sem.at[m], wp_r.at[0], ee=partner).wait_send()

    def finish(c):
        cols = slice(c * wide, (c + 1) * wide)

        for r in halves:
            @when(z > 0)
            def _():
                zd_copy(z, z, c, r, above).wait_recv()

            @when(z < Z - 1)
            def _():
                zd_copy(z, Z, c, r, above).wait_recv()

        for i in range(T // trow):
            rows = slice(i * trow, (i + 1) * trow)
            total = pd[z, rows, cols].astype(f32) + rpd[z, rows, cols].astype(f32) + rpd[Z, rows, cols].astype(f32)
            out[rows, cols] = (base[rows, cols] + total).astype(bf16)

    per = SUBS[1] // nk
    def along(kind):
        for i, c, r in kind:
            zd_pass(i, c, r)

    def in_turn(first_kind, second_kind):
        if not lined:
            return

        @when(turn == 0)
        def _():
            along(first_kind)

        @when(turn == 1)
        def _():
            along(second_kind)

    near, far = list(range(mine, Z)), list(range(mine))
    n0, n1, f0 = near[0], near[1:], far[0] if far else 0

    def both(items, c):
        return [(i, c, r) for i in items for r in halves]

    def rest_of(items, c):
        return [(i, c, r) for i in items for r in halves[1:]]


    def mlp_hidden(group, i, n):
        rows = slice(group[0] * tall, (group[-1] + 1) * tall)
        hidden(lambda: normed[rows, :], len(group) * tall, win, *part_of(i, n), at=group[0] * tall)

    groups = [halves[:1], halves[1:]] if lined else [halves]
    mlp_hidden(groups[0], 0, 2)
    take(point(10))
    mlp_hidden(groups[0], 1, 2)
    locals_[4].wait()
    own_copies[1].wait_recv()
    if lined:
        dense(0, 0, groups[0])
        dense(0, 1, groups[0])
    weights(11, 9)
    passes(zo_far, fast, 1)
    for t in range(2, Z - 1):
        passes(zo_near, fast, t)
        passes(zo_far, fast, t)
    if lined:
        mlp_hidden(groups[1], 0, 2)
        relay(point(10))
        passes(zo_near, slow, 0)
        mlp_hidden(groups[1], 1, 2)
        dense(0, 0, groups[1])
        weights(12, 11)
        dense(1, 0)
    else:
        weights(12, 10)
        passes(zo_near, slow, 0)
        weights(13, 11)
        for i in range(mine):
            dense(i, 0)
    relay(point(12))
    passes(zo_near, slow, 1)
    passes(zo_far, slow, 0)
    in_turn([], [(f0, 0, 0)])
    if nk > 1:
        collect(1)
        for i in range(mine, Z):
            dense(i, 0)
            take(point(13))
        passes(zo_far, slow, 1)
        for q in fast:
            zo_final(q)
            ret_copy(q).start()
        in_turn([(n0, 0, 0)], [(f0, 1, 0)] + rest_of([f0], 0))
        for c in range(1, nk):
            for i in range(mine):
                dense(i, c, groups[-1] if i == 0 else halves)
                take(point(14))
    weights(15, 13)
    for t in range(1 if nk == 1 else 2, Z - 1):
        passes(zo_near, slow, t)
        passes(zo_far, slow, t)
    for q in slow if nk > 1 else units:
        zo_final(q)
        ret_copy(q).start()
    in_turn(rest_of([n0], 0), both(far[1:], 0))
    relay(point(14))
    weights(16, 15)
    in_turn([(i, 0, 0) for i in n1[:1]], [(n0, 0, 0)])
    relay(point(16))
    collect(nk)
    for i in range(mine, Z):
        dense(i, nk - 1)
        if i == mine:
            in_turn(rest_of(n1[:1], 0), rest_of([n0], 0))
    for c in range(nk):
        for i in range(Z):
            for r in halves:
                dense_edge(i, c, r, True, slice_number(i))
    in_turn(both(far, 0) + both(n1[1:], 0), both(n1, 0))
    if not lined:
        along([(i, 0, r) for i in range(Z) for r in halves])
    combine_experts()
    in_turn([(f0, 1, 0), (n0, 1, 0)], rest_of([f0], 1))
    sent()
    in_turn(rest_of([n0], 1) + rest_of([f0], 1) + both(far[1:], 1) + both(n1, 1),
            both(far[1:], 1) + both(near, 1))
    if not lined:
        along([(i, c, r) for c in range(1, nk) for i in range(Z) for r in halves])
    for c in range(nk):
        finish(c)

    def last_waits():
        for array, sem in ((po, zo_s), (pd, zd_s)):
            part = array.at[pl.ds(0, Z - 1)]
            remote(part, part, sem.at[0], wp_r.at[0], ee=partner).wait_send()

    last_waits()


def local(tokens, route, gate_prob, norm_gain, dense_in, dense_out, expert_in, expert_out):
    G, E, Z = lax.axis_size("groups"), lax.axis_size("expert"), lax.axis_size("cuts")
    T, D = tokens.shape
    F = dense_in.shape[1]
    share = D // Z
    De = D // E
    cap = max(2, 3 * T // (2 * E))
    C = E // 2
    away = E - 2
    others = away * cap
    nk = 2 if De == share and share % 256 == 0 else 1
    bf16 = jnp.bfloat16
    any_, vmem = pl.BlockSpec(memory_space=pl.ANY), pl.BlockSpec(memory_space=pltpu.VMEM)
    dma = pltpu.SemaphoreType.DMA
    splits = (max(1, min(8, De // (16 * G))), 8)
    subs = max(splits)
    return pl.pallas_call(
        functools.partial(kernel, G, E, Z, cap, nk, splits),
        out_shape=jax.ShapeDtypeStruct((T, share), bf16),
        in_specs=[any_, any_, any_, any_, any_, any_, any_, any_],
        out_specs=vmem,
        scratch_shapes=[
            pltpu.VMEM((D, F), bf16), pltpu.VMEM((F, D), bf16),
            pltpu.VMEM((D, F), bf16), pltpu.VMEM((F, D), bf16),
            pltpu.VMEM((T, D), bf16), pltpu.VMEM((T, D), bf16),
            pltpu.VMEM((2, others, share), bf16), pltpu.VMEM((cap, D), bf16), pltpu.VMEM((E * cap, D), bf16),
            pltpu.VMEM((max(T, 3 * cap), F), bf16),
            pltpu.VMEM((2 * cap, D), bf16), pltpu.VMEM((cap, D), bf16),
            pltpu.VMEM((Z, others, share), bf16), pltpu.VMEM((Z + 1, others, share), bf16),
            pltpu.VMEM((Z, T, share), bf16), pltpu.VMEM((Z + 1, T, share), bf16),
            pltpu.VMEM((others, share), bf16), pltpu.VMEM((others, share), bf16),
            pltpu.VMEM((T, share), jnp.float32), pltpu.VMEM((T, 2 * cap), bf16),
            pltpu.VMEM((T, 128), jnp.float32), pltpu.VMEM((T, D), bf16), pltpu.VMEM((cap, F), jnp.float32),
            pltpu.VMEM((1, T), jnp.int32), pltpu.VMEM((1, T), jnp.float32), pltpu.VMEM((1, D), jnp.float32),
            dma((12,)), dma((2,)), dma((2,)), dma((1,)), dma((1,)), dma((away, 2)), dma((away, 2)),
            dma((away, 2, Z - 1)), dma((away, 2, Z - 1)), dma((1,)), dma((1,)),
            dma((2,)), dma((2, C - 1, subs + nk * (G - 1))), dma((2,)), dma((2, C - 1, subs, G - 1)), dma((2,)), dma((1 + nk,)),
            dma((1,)), dma((away, Z + 1)), dma((1,)), dma((Z + 1, 2 * nk)), dma((away,)), dma((away,)),
        ],
        compiler_params=pltpu.CompilerParams(
            collective_id=0, has_side_effects=True, vmem_limit_bytes=67043328
        ),
    )(tokens, route.reshape(1, T), gate_prob[None, :], norm_gain[None, :], dense_in, dense_out, expert_in, expert_out)


def solution(mesh):
    return jax.shard_map(
        local,
        mesh=mesh,
        in_specs=(
            P(("groups", "expert"), None),
            P(("groups", "expert"), None),
            P(("groups", "expert")),
            P(),
            P("expert", "cuts"),
            P("cuts", "expert"),
            P("expert", None, "cuts"),
            P("expert", "cuts", None),
        ),
        out_specs=P(("groups", "expert"), "cuts"),
        check_vma=False,
    )
```

```python
import functools

import jax
import jax.numpy as jnp
from jax import lax
from jax.experimental import pallas as pl
from jax.experimental.pallas import tpu as pltpu
from jax.sharding import PartitionSpec as P


def kernel(G, E, Z, cap, nk, SUBS, tokens, route_h, gate_h, gain_h, din, dout, ein_h, eout_h, out,
           win, wout, ein, eout, tok, normed, disp, dispq, arrived, hbuf, pown, psend, po, rpo, pd, rpd,
           ret, rret, base, pk, turned, eres, acc, route, gate, gain,
           loc, own_s, own_r, d1_s, d1_r, dx_s, dx_r, ag_s, ag_r, pq_s, pq_r,
           wx_s, wx_r, wy_s, wy_r, wp_s, wp_r, zo_s, zo_r, zd_s, zd_r, ret_s, ret_r):
    f32, bf16 = jnp.float32, jnp.bfloat16
    T, D = tok.shape
    F = ein.shape[1]
    De = D // E
    share = D // Z
    C = E // 2
    wide = share // nk
    tn = min(256, wide)
    units = range(2, E)
    fast, slow = units[:(E - 2) // 2], units[(E - 2) // 2:]
    g, e, z = lax.axis_index("groups"), lax.axis_index("expert"), lax.axis_index("cuts")
    chip, core = e // 2, lax.rem(e, 2)
    partner = chip * 2 + 1 - core
    above, below = lax.rem(z + 1, Z), lax.rem(z + Z - 1, Z)
    upper = (2 * z) // Z

    def remote(src, dst, send, recv, gg=None, ee=None, zz=None):
        return pltpu.make_async_remote_copy(
            src_ref=src, dst_ref=dst, send_sem=send, recv_sem=recv,
            device_id={
                "groups": g if gg is None else gg,
                "expert": e if ee is None else ee,
                "cuts": z if zz is None else zz,
            },
            device_id_type=pl.DeviceIdType.MESH,
        )

    def when(condition):
        return pl.when(condition)

    def expert_at(kc, j):
        other = lax.rem(chip + kc + C, C)
        return other * 2 + (core if j == 0 else 1 - core)

    my_rows = pl.ds(pl.multiple_of(e * De, De), De)
    locals_ = [
        pltpu.make_async_copy(route_h, route, loc.at[0]),
        pltpu.make_async_copy(ein_h.at[0], ein, loc.at[1]),
        pltpu.make_async_copy(eout_h.at[0], eout, loc.at[2]),
        pltpu.make_async_copy(din, win.at[my_rows, :], loc.at[3]),
        pltpu.make_async_copy(dout, wout.at[:, my_rows], loc.at[4]),
    ]
    chunks = 4 if T % 256 == 0 else 1
    loads = []
    for k in range(chunks):
        part = pl.ds(k * (T // chunks), T // chunks)
        loads.append(pltpu.make_async_copy(tokens.at[part, :], tok.at[part, :], loc.at[5 + k]))
    small = [
        pltpu.make_async_copy(gain_h, gain, loc.at[9]),
        pltpu.make_async_copy(gate_h, gate, loc.at[10]),
        locals_[0],
    ]
    for copy in small + loads:
        copy.start()

    barrier = pltpu.get_barrier_semaphore()
    for k in range(1, E):
        pl.semaphore_signal(barrier, inc=1, device_id={"groups": g, "expert": lax.rem(e + k, E), "cuts": z},
                            device_id_type=pl.DeviceIdType.MESH)
    for k in range(1, Z):
        pl.semaphore_signal(barrier, inc=1, device_id={"groups": g, "expert": e, "cuts": lax.rem(z + k, Z)},
                            device_id_type=pl.DeviceIdType.MESH)
    for k in range(1, G):
        pl.semaphore_signal(barrier, inc=1, device_id={"groups": lax.rem(g + k, G), "expert": e, "cuts": z},
                            device_id_type=pl.DeviceIdType.MESH)

    own_copies = [
        remote(din, win.at[my_rows, :], own_s.at[0], own_r.at[0], ee=partner),
        remote(dout, wout.at[:, my_rows], own_s.at[1], own_r.at[1], ee=partner),
    ]

    def block(m, p, s):
        if m == 0:
            n = De // G // SUBS[0]
            return p * (De // G) + s * n, n, 0, F
        per = SUBS[1] // nk
        n = F // G // per
        return p * (F // G) + (s % per) * n, n, (s // per) * (De // nk), De // nk

    def weight(m, owner, p, s):
        row, n, col, width = block(m, p, s)
        if m == 0:
            return win.at[pl.ds(pl.multiple_of(owner * De + row, n), n), :]
        return wout.at[pl.ds(pl.multiple_of(row, n), n),
                       pl.ds(pl.multiple_of(owner * De + col, width), width)]

    def weight_source(m, p, s):
        row, n, col, width = block(m, p, s)
        return (din, dout)[m].at[pl.ds(pl.multiple_of(row, n), n), pl.ds(col, width)]

    def direct(m, s):
        per = SUBS[0] if m == 0 else SUBS[1] // nk
        return per > 1 and s % per == per - 1

    def x_copy(m, kc, s, dg=0):
        half = lax.rem(g - dg + G, G)
        group = s // (SUBS[1] // nk) if m else 0
        place = s if dg == 0 else max(SUBS) + group * (G - 1) + dg - 1
        return remote(weight_source(m, half, s), weight(m, e, half, s), wx_s.at[m],
                      wx_r.at[m, kc - 1, place], ee=expert_at(kc, 0))

    def y_copy(m, kc, s, dg):
        w = weight(m, expert_at(-kc, 0), g, s)
        return remote(w, w, wy_s.at[m], wy_r.at[m, kc - 1, s, dg - 1], gg=lax.rem(g + dg, G))

    def p_copy(m, kc, s, dg):
        w = weight(m, expert_at(-kc, 0), lax.rem(g - dg + G, G), s)
        return remote(w, w, wp_s.at[m], wp_r.at[m * (1 + s // (SUBS[1] // nk))], ee=partner)

    steps = [(m, s) for m in range(2) for s in range(SUBS[m])]
    issued, taken, relayed = [0], [0], [0]

    def issue(upto):
        while issued[0] < min(upto, len(steps)):
            m, s = steps[issued[0]]
            for kc in range(1, C):
                for dg in range(G if direct(m, s) else 1):
                    x_copy(m, kc, s, dg).start()
            issued[0] += 1

    def relay(upto):
        while relayed[0] < min(upto, taken[0]):
            m, s = steps[relayed[0]]
            for kc in range(1, C):
                for dg in range(1, 1 if direct(m, s) else G):
                    y_copy(m, kc, s, dg).wait_recv()
                    p_copy(m, kc, s, dg).start()
            relayed[0] += 1

    def take(upto):
        while taken[0] < min(upto, len(steps)):
            m, s = steps[taken[0]]
            for kc in range(1, C):
                for dg in range(G if direct(m, s) else 1):
                    x_copy(m, kc, s, dg).wait_recv()
                for dg in range(1, 1 if direct(m, s) else G):
                    y_copy(m, kc, s, dg).start()
                for dg in range(G if direct(m, s) else 1):
                    p_copy(m, kc, s, dg).start()
            taken[0] += 1

    def weight_part(m, rows, cols):
        return (win, wout)[m].at[pl.ds(0, rows), pl.ds(0, cols)]

    def collect(n):
        w = weight_part(1, F, (C - 1) * De // nk) if n else weight_part(0, (C - 1) * De, F)
        remote(w, w, wp_s.at[0], wp_r.at[n], ee=partner).wait_recv()

    for copy in small:
        copy.wait()

    nrow = min(64, T)

    def norm_step(i, carry):
        rows = pl.ds(pl.multiple_of(i * nrow, nrow), nrow)
        x = tok[rows, :].astype(f32)
        ms = jnp.mean(x * x, axis=-1, keepdims=True)
        normed[rows, :] = (x * lax.rsqrt(ms + 1e-06) * gain[...]).astype(bf16)
        return carry

    for k in range(chunks):
        loads[k].wait()
        if k == chunks - 1:
            for copy in locals_[1:]:
                copy.start()
        lax.fori_loop(k * (T // nrow) // chunks, (k + 1) * (T // nrow) // chunks, norm_step, 0)

    picked = route[...]
    lanes = -(-E // 8) * 8
    one_hot = (lax.broadcasted_iota(jnp.int32, (lanes, T), 0) == picked).astype(f32)
    earlier = (lax.broadcasted_iota(jnp.int32, (T, T), 0) < lax.broadcasted_iota(jnp.int32, (T, T), 1))
    before = jnp.dot(one_hot.astype(bf16), earlier.astype(f32).astype(bf16), preferred_element_type=f32)
    position = jnp.sum(before * one_hot, axis=0, keepdims=True)
    slot_row = picked.astype(f32) * float(cap) + position

    def slice_at(s):
        return pl.ds(pl.multiple_of(s * share, share), share)

    def picks(q):
        dest = expert_at(q // 2, q % 2)
        wanted = slot_row - (dest * cap).astype(f32)
        return (lax.broadcasted_iota(jnp.int32, (cap, T), 0).astype(f32) == wanted).astype(f32).astype(bf16)

    def fill_slice(q, x, s):
        disp[x, (q - 2) * cap:(q - 1) * cap, :] = jnp.dot(
            picks(q), normed[:, slice_at(s)], preferred_element_type=f32).astype(bf16)

    def fill(q, dst):
        pick = picks(q)
        dn = min(512, D)

        def step(i, carry):
            cols = pl.ds(pl.multiple_of(i * dn, dn), dn)
            dst[0:cap, cols] = jnp.dot(pick, normed[:, cols], preferred_element_type=f32).astype(bf16)
            return carry

        lax.fori_loop(0, D // dn, step, 0)

    ends = ((0, Z - 1), (Z - 1, 0))

    def dx_copy(q, x, s):
        return remote(disp.at[x, pl.ds((q - 2) * cap, cap), :], arrived.at[pl.ds(q * cap, cap), slice_at(s)],
                      dx_s.at[q - 2, x], dx_r.at[q - 2, x], ee=expert_at(q // 2, q % 2))

    d1_copy = remote(dispq, arrived.at[pl.ds(cap, cap), :], d1_s.at[0], d1_r.at[0], ee=partner)

    for q in units:
        fill_slice(q, 0, z)
    pl.semaphore_wait(barrier, (E - 1) + (Z - 1) + (G - 1))
    for q in units:
        dx_copy(q, 0, z).start()
    for at, s in ends:
        @when(z == at)
        def _():
            for q in fast:
                fill_slice(q, 1, s)
    fill(1, dispq)
    for at, s in ends:
        @when(z == at)
        def _():
            for q in fast:
                dx_copy(q, 1, s).start()
    issue(len(steps))
    fill(0, arrived)
    d1_copy.start()
    for copy in own_copies:
        copy.start()

    def hop(q, way, t, s):
        part = arrived.at[pl.ds(q * cap, cap), slice_at(s)]
        return remote(part, part, ag_s.at[q - 2, way, t - 1], ag_r.at[q - 2, way, t - 1], zz=below if way else above)

    def hops(q):
        return Z - 2 if q in fast else Z - 1

    def gather(q, t, middle=True, edges=True):
        if t == 0:
            dx_copy(q, 0, z).wait_recv()
        inner = (z > 0) & (z < Z - 1)
        here = True if middle and edges else inner if middle else ~inner

        @when((z >= t) & here)
        def _():
            if t > 0:
                hop(q, 0, t, z - t).wait_recv()
        if t < hops(q) and middle:
            @when((z >= t) & (z < Z - 1))
            def _():
                hop(q, 0, t + 1, z - t).start()

        @when((z + t <= Z - 1) & here)
        def _():
            if t > 0:
                hop(q, 1, t, z + t).wait_recv()
        if t < hops(q) and middle:
            @when((z + t <= Z - 1) & (z > 0))
            def _():
                hop(q, 1, t + 1, z + t).start()

    def hidden(load, rows, w, lo=0, hi=None, at=0):
        def step(i, carry):
            cols = pl.ds(pl.multiple_of(i * 256, 256), 256)
            product = jnp.dot(load(), w[:, cols], preferred_element_type=f32)
            hbuf[at:at + rows, cols] = jax.nn.gelu(product).astype(bf16)
            return carry

        lax.fori_loop(lo, F // 256 if hi is None else hi, step, 0)

    blocks = F // 256

    def part_of(i, n):
        return i * blocks // n, (i + 1) * blocks // n

    pair = 2 * cap
    first_row = lax.broadcasted_iota(jnp.int32, (128, T), 0) == 0
    turned[...] = jnp.transpose(jnp.where(first_row, slot_row, gate[...]))
    slot_col = turned[:, 0:1]
    col = lax.broadcasted_iota(jnp.int32, (T, pair), 1).astype(f32)
    here = slot_col - (e * cap).astype(f32)
    there = slot_col - (partner * cap).astype(f32) + float(cap)
    pk[...] = (((col == here) & (col < cap)) | ((col == there) & (col >= cap))).astype(f32).astype(bf16)

    locals_[1].wait()
    d1_copy.wait_recv()
    for i in range(4):
        hidden(lambda: arrived[0:pair, :], pair, ein, *part_of(i, 4))
        if i == 1:
            for q in fast:
                gather(q, 0)
    for q in slow:
        gather(q, 0)

    locals_[2].wait()

    def own_step(i, carry):
        cols = pl.ds(pl.multiple_of(i * 256, 256), 256)
        acc = jnp.dot(hbuf[0:pair, :], eout[:, cols], preferred_element_type=f32).astype(bf16)
        pown[0:cap, cols] = acc[0:cap, :]
        psend[:, cols] = acc[cap:pair, :]
        return carry

    own_blocks = D // 256
    lax.fori_loop(0, own_blocks // 2, own_step, 0)

    ahead = Z == 4 and len(fast) == 1
    last_fast, last_slow = lax.rem(z + 2, Z), (Z - 1) * (1 - upper)

    def take_extra(q):
        for at, s in ends:
            @when(z == at)
            def _():
                dx_copy(q, 1, s).wait_recv()

    def slice_dot(q, s, cols):
        return jnp.dot(arrived[q * cap:(q + 1) * cap, slice_at(s)], ein[slice_at(s), cols],
                       preferred_element_type=f32)

    def multiply_ahead(q, last):
        def step(i, carry):
            cols = pl.ds(pl.multiple_of(i * 256, 256), 256)
            acc[:, cols] = sum(slice_dot(q, lax.rem(last + k, Z), cols) for k in range(1, Z))
            return carry

        lax.fori_loop(0, blocks, step, 0)

    def multiply_last(q, last, at):
        def step(i, carry):
            cols = pl.ds(pl.multiple_of(i * 256, 256), 256)
            hbuf[at:at + cap, cols] = jax.nn.gelu(acc[:, cols] + slice_dot(q, last, cols)).astype(bf16)
            return carry

        lax.fori_loop(0, blocks, step, 0)

    if Z > 2:
        for q in fast:
            gather(q, 1)
    if ahead:
        take_extra(fast[0])
        multiply_ahead(fast[0], last_fast)
    if Z > 2:
        for q in slow:
            gather(q, 1)

    def own_rest():
        lax.fori_loop(own_blocks // 2, own_blocks, own_step, 0)
        pq_copy.start()

    @when(z == 0)
    def _():
        rpo[0] = jnp.zeros(rpo.shape[1:], bf16)
        rpd[0] = jnp.zeros(rpd.shape[1:], bf16)

    @when(z == Z - 1)
    def _():
        rpo[Z] = jnp.zeros(rpo.shape[1:], bf16)
        rpd[Z] = jnp.zeros(rpd.shape[1:], bf16)

    pq_copy = remote(psend, pown.at[pl.ds(cap, cap), :], pq_s.at[0], pq_r.at[0], ee=partner)
    if not ahead:
        own_rest()

    def zo_copy(q, d, slot, to):
        rows = pl.ds((q - 2) * cap, cap)
        return remote(po.at[d, rows, :], rpo.at[slot, rows, :], zo_s.at[0], zo_r.at[q - 2, slot], zz=to)

    def back_slot(d, to):
        return Z if d == to else d

    def zo_edge(q, i):
        @when(z == 0)
        def _():
            zo_copy(q, Z - 1 - i, Z - 1 - i, 1).start()

        @when(z == Z - 1)
        def _():
            zo_copy(q, i, back_slot(i, Z - 2), Z - 2).start()

    def expert_hidden(q, between=None):
        if q in fast:
            take_extra(q)
        rows = slice(q * cap, (q + 1) * cap)
        hidden(lambda: arrived[rows, :], cap, ein, *part_of(0, 2))
        if between is not None:
            between()
        hidden(lambda: arrived[rows, :], cap, ein, *part_of(1, 2))

    def expert_out(q, between=None, at=0):
        rows = slice((q - 2) * cap, (q - 1) * cap)
        for i in range(Z):
            d = (1 - upper) * (Z - 1 - i) + upper * i

            def step(k, carry):
                acc = jnp.dot(hbuf[at:at + cap, :], eout[:, pl.ds(pl.multiple_of(d * share + k * 256, 256), 256)],
                              preferred_element_type=f32)
                po[d, rows, pl.ds(pl.multiple_of(k * 256, 256), 256)] = acc.astype(bf16)
                return carry

            lax.fori_loop(0, share // 256, step, 0)
            if i < Z - 1:
                zo_edge(q, i)
            if between is not None:
                between(i)

    def zo_up(q, d):
        @when((z > 0) & (z < d))
        def _():
            rows = slice((q - 2) * cap, (q - 1) * cap)
            zo_copy(q, d, d, above).wait_recv()
            po[d, rows, :] = (po[d, rows, :].astype(f32) + rpo[d, rows, :].astype(f32)).astype(bf16)
            zo_copy(q, d, d, above).start()

    def zo_down(q, d):
        @when((z < Z - 1) & (z > d))
        def _():
            rows = slice((q - 2) * cap, (q - 1) * cap)
            zo_copy(q, d, d, below).wait_recv()
            po[d, rows, :] = (po[d, rows, :].astype(f32) + rpo[d, rows, :].astype(f32)).astype(bf16)

        for slot, near in ((d, z > d + 1), (Z, z == d + 1)):
            @when((z < Z - 1) & near)
            def _():
                zo_copy(q, d, slot, below).start()

    def zo_near(q, t):
        @when(upper == 0)
        def _():
            zo_up(q, Z - 1 - t)

        @when(upper == 1)
        def _():
            zo_down(q, t)

    def zo_far(q, t):
        @when(upper == 0)
        def _():
            zo_down(q, t)

        @when(upper == 1)
        def _():
            zo_up(q, Z - 1 - t)

    def ret_copy(q):
        rows = pl.ds((q - 2) * cap, cap)
        return remote(ret.at[rows, :], rret.at[rows, :], ret_s.at[q - 2], ret_r.at[q - 2], ee=expert_at(-(q // 2), q % 2))

    def zo_final(q):
        @when(z > 0)
        def _():
            zo_copy(q, z, z, above).wait_recv()

        @when(z < Z - 1)
        def _():
            zo_copy(q, z, Z, above).wait_recv()
        rows = slice((q - 2) * cap, (q - 1) * cap)
        ret[rows, :] = (po[z, rows, :].astype(f32) + rpo[z, rows, :].astype(f32)
                        + rpo[Z, rows, :].astype(f32)).astype(bf16)

    def point(n):
        return n * SUBS[0] // 8 if n <= 8 else SUBS[0] + (n - 8) * SUBS[1] // 8

    def weights(to_take, to_relay):
        take(point(to_take))
        relay(point(to_relay))

    def passes(kind, group, t):
        if t < Z - 1:
            for q in group:
                kind(q, t)

    take(point(1))
    for t in range(2, Z - 1):
        for q in fast:
            gather(q, t)
    take(point(2))

    def slow_hops():
        for k in slow:
            for t in range(2, Z - 1):
                gather(k, t, edges=t == 0)

    def serve_fast(i):
        if i == 0:
            take(point(3))
        if i == 1:
            slow_hops()
        if i == Z - 1:
            take(point(4))

    if ahead:
        multiply_last(fast[0], last_fast, pair)
        expert_out(fast[0], serve_fast, pair)
        own_rest()
    else:
        for n, q in enumerate(fast):
            expert_hidden(q)
            expert_out(q, serve_fast if n == len(fast) - 1 else None)
    weights(5, 2)

    def own_rows(i, carry):
        cols = pl.ds(pl.multiple_of(i * 256, 256), 256)
        res = jnp.dot(pk[...], pown[:, cols], preferred_element_type=f32)
        eres[:, cols] = (turned[:, 1:2] * res).astype(bf16)
        return carry

    def serve_hidden():
        weights(7, 4)
        passes(zo_near, fast, 0)

    def serve(i):
        if i == Z // 2:
            relay(point(6))

    for n, q in enumerate(slow):
        final = n == len(slow) - 1
        for t in range(2, Z - 1):
            gather(q, t, middle=False)
        if ahead:
            multiply_ahead(q, last_slow)
        gather(q, Z - 1)
        if n == 0:
            weights(6, 3)
        if ahead:
            multiply_last(q, last_slow, 0)
            serve_hidden()
        else:
            expert_hidden(q, serve_hidden if final else None)
        if final:
            relay(point(5))
        expert_out(q, serve if final else None)
    passes(zo_near, fast, 1)
    take(point(8))
    pq_copy.wait_recv()
    lax.fori_loop(0, own_blocks, own_rows, 0)
    relay(point(7))
    passes(zo_far, fast, 0)
    relay(point(8))
    locals_[3].wait()
    own_copies[0].wait_recv()
    collect(0)
    take(point(9))

    nr = 2 if T % 32 == 0 else 1
    tall = T // nr
    halves = range(nr)

    def zd_copy(d, slot, c, r, to):
        rows, cols = pl.ds(r * tall, tall), pl.ds(c * wide, wide)
        n = c * nr + r
        return remote(pd.at[d, rows, cols], rpd.at[slot, rows, cols], zd_s.at[0], zd_r.at[slot, n], zz=to)

    mine = Z // C if Z % C == 0 else 0
    lined = C == 2 and nk == 2 and mine > 1
    turn = lax.rem(upper + chip, 2)

    def slice_number(i):
        if C == 2 and Z % 2 == 0:
            low = i if i < mine else Z - 1 - (i - mine)
            return chip * (Z - 1 - low) + (1 - chip) * low
        return lax.rem(chip * mine + i, Z)

    def late(i, c, r):
        return c == nk - 1 and r == nr - 1 and lined and i < mine

    def dense(i, c, group=None):
        group = halves if group is None else group
        d = slice_number(i)
        rows = slice(group[0] * tall, (group[-1] + 1) * tall)
        if lined and i < mine:
            d = turn * d + (1 - turn) * slice_number(mine - 1 - i)

        def step(k, carry):
            cols = pl.ds(pl.multiple_of(d * share + c * wide + k * tn, tn), tn)
            acc = jnp.dot(hbuf[rows, :], wout[:, cols], preferred_element_type=f32)
            pd[d, rows, pl.ds(pl.multiple_of(c * wide + k * tn, tn), tn)] = (acc + eres[rows, cols].astype(f32)).astype(bf16)
            return carry

        lax.fori_loop(0, wide // tn, step, 0)

        for r in group:
            dense_edge(i, c, r, False, d)

    def dense_edge(i, c, r, again, d):
        beside = ((z == 0) & (d == 1)) | ((z == Z - 1) & (d == Z - 2))
        go = (beside if again else ~beside) if late(i, c, r) else True
        if again and not late(i, c, r):
            return

        @when((z == 0) & (d > 0) & go)
        def _():
            zd_copy(d, d, c, r, above).start()

        for slot, near in ((d, z > d + 1), (Z, z == d + 1)):
            @when((z == Z - 1) & near & go)
            def _():
                zd_copy(d, slot, c, r, below).start()

    def zd_pass(i, c, r):
        d = slice_number(i)
        rows, cols = pl.ds(r * tall, tall), pl.ds(c * wide, wide)

        @when((z > 0) & (z < Z - 1) & (z != d))
        def _():
            zd_copy(d, d, c, r, above).wait_recv()
            pd[d, rows, cols] = (pd[d, rows, cols].astype(f32) + rpd[d, rows, cols].astype(f32)).astype(bf16)

        @when((z > 0) & (z < d))
        def _():
            zd_copy(d, d, c, r, above).start()

        for slot, near in ((d, z > d + 1), (Z, z == d + 1)):
            @when((z < Z - 1) & near)
            def _():
                zd_copy(d, slot, c, r, below).start()

    trow = min(128, T)
    residual = slice_at(z)

    def combine_experts():
        for q in units:
            ret_copy(q).wait_recv()
        for i in range(T // trow):
            rows = slice(i * trow, (i + 1) * trow)
            res = jnp.zeros((trow, share), f32)
            for q in units:
                wanted = turned[rows, 0:1] - (expert_at(q // 2, q % 2) * cap).astype(f32)
                pick = (lax.broadcasted_iota(jnp.int32, (trow, cap), 1).astype(f32) == wanted)
                res = res + jnp.dot(pick.astype(f32).astype(bf16), rret[(q - 2) * cap:(q - 1) * cap, :],
                                    preferred_element_type=f32)
            base[rows, :] = tok[rows, residual].astype(f32) + turned[rows, 1:2] * res

    def sent():
        for copy in own_copies:
            copy.wait_send()
        d1_copy.wait_send()
        pq_copy.wait_send()
        for q in units:
            dx_copy(q, 0, z).wait_send()
            ret_copy(q).wait_send()
            for at, s in ends:
                @when((z == at) & (q in fast))
                def _():
                    dx_copy(q, 1, s).wait_send()
            for t in range(1, hops(q) + 1):
                @when((z >= t - 1) & (z < Z - 1))
                def _():
                    hop(q, 0, t, z - t + 1).wait_send()

                @when((z + t - 1 <= Z - 1) & (z > 0))
                def _():
                    hop(q, 1, t, z + t - 1).wait_send()
        for m in range(2):
            for sem, n in ((wx_s, 1), (wy_s, G - 1), (wp_s, G)):
                rows, cols = ((C - 1) * De // G * n, F) if m == 0 else (F // G * n, (C - 1) * De)
                if direct(m, SUBS[m] - 1) and sem is not wp_s:
                    extra = (C - 1) * (G - 1) * De // G // SUBS[0] if m == 0 else (G - 1) * F // G // (SUBS[1] // nk)
                    rows += extra if sem is wx_s else -extra
                w = weight_part(m, rows, cols)
                remote(w, w, sem.at[m], wp_r.at[0], ee=partner).wait_send()

    def finish(c):
        cols = slice(c * wide, (c + 1) * wide)

        for r in halves:
            @when(z > 0)
            def _():
                zd_copy(z, z, c, r, above).wait_recv()

            @when(z < Z - 1)
            def _():
                zd_copy(z, Z, c, r, above).wait_recv()

        for i in range(T // trow):
            rows = slice(i * trow, (i + 1) * trow)
            total = pd[z, rows, cols].astype(f32) + rpd[z, rows, cols].astype(f32) + rpd[Z, rows, cols].astype(f32)
            out[rows, cols] = (base[rows, cols] + total).astype(bf16)

    per = SUBS[1] // nk
    def along(kind):
        for i, c, r in kind:
            zd_pass(i, c, r)

    def in_turn(first_kind, second_kind):
        if not lined:
            return

        @when(turn == 0)
        def _():
            along(first_kind)

        @when(turn == 1)
        def _():
            along(second_kind)

    near, far = list(range(mine, Z)), list(range(mine))
    n0, n1, f0 = near[0], near[1:], far[0] if far else 0

    def both(items, c):
        return [(i, c, r) for i in items for r in halves]

    def rest_of(items, c):
        return [(i, c, r) for i in items for r in halves[1:]]


    def mlp_hidden(group, i, n):
        rows = slice(group[0] * tall, (group[-1] + 1) * tall)
        hidden(lambda: normed[rows, :], len(group) * tall, win, *part_of(i, n), at=group[0] * tall)

    groups = [halves[:1], halves[1:]] if lined else [halves]
    mlp_hidden(groups[0], 0, 2)
    take(point(10))
    mlp_hidden(groups[0], 1, 2)
    locals_[4].wait()
    own_copies[1].wait_recv()
    if lined:
        dense(0, 0, groups[0])
        dense(0, 1, groups[0])
    weights(11, 9)
    passes(zo_far, fast, 1)
    for t in range(2, Z - 1):
        passes(zo_near, fast, t)
        passes(zo_far, fast, t)
    if lined:
        mlp_hidden(groups[1], 0, 2)
        relay(point(10))
        passes(zo_near, slow, 0)
        mlp_hidden(groups[1], 1, 2)
        dense(0, 0, groups[1])
        weights(12, 11)
        dense(1, 0)
    else:
        weights(12, 10)
        passes(zo_near, slow, 0)
        weights(13, 11)
        for i in range(mine):
            dense(i, 0)
    relay(point(12))
    passes(zo_near, slow, 1)
    passes(zo_far, slow, 0)
    in_turn([], [(f0, 0, 0)])
    if nk > 1:
        collect(1)
        for i in range(mine, Z):
            dense(i, 0)
            take(point(13))
        passes(zo_far, slow, 1)
        for q in fast:
            zo_final(q)
            ret_copy(q).start()
        in_turn([], [(f0, 1, 0)] + rest_of([f0], 0))
        for c in range(1, nk):
            for i in range(mine):
                dense(i, c, groups[-1] if i == 0 else halves)
                take(point(14))
    in_turn([(n0, 0, 0)], [])
    weights(15, 13)
    for t in range(1 if nk == 1 else 2, Z - 1):
        passes(zo_near, slow, t)
        passes(zo_far, slow, t)
    for q in slow if nk > 1 else units:
        zo_final(q)
        ret_copy(q).start()
    in_turn(rest_of([n0], 0), both(far[1:], 0))
    relay(point(14))
    weights(16, 15)
    in_turn([(i, 0, 0) for i in n1[:1]], [(n0, 0, 0)])
    relay(point(16))
    collect(nk)
    for i in range(mine, Z):
        dense(i, nk - 1)
        if i == mine:
            in_turn(rest_of(n1[:1], 0), rest_of([n0], 0))
    for c in range(nk):
        for i in range(Z):
            for r in halves:
                dense_edge(i, c, r, True, slice_number(i))
    in_turn(both(far, 0) + both(n1[1:], 0), both(n1, 0))
    if not lined:
        along([(i, 0, r) for i in range(Z) for r in halves])
    combine_experts()
    in_turn([(f0, 1, 0), (n0, 1, 0)], rest_of([f0], 1))
    sent()
    in_turn(rest_of([n0], 1) + rest_of([f0], 1) + both(far[1:], 1) + both(n1, 1),
            both(far[1:], 1) + both(near, 1))
    if not lined:
        along([(i, c, r) for c in range(1, nk) for i in range(Z) for r in halves])
    for c in range(nk):
        finish(c)

    def last_waits():
        for array, sem in ((po, zo_s), (pd, zd_s)):
            part = array.at[pl.ds(0, Z - 1)]
            remote(part, part, sem.at[0], wp_r.at[0], ee=partner).wait_send()

    last_waits()


def local(tokens, route, gate_prob, norm_gain, dense_in, dense_out, expert_in, expert_out):
    G, E, Z = lax.axis_size("groups"), lax.axis_size("expert"), lax.axis_size("cuts")
    T, D = tokens.shape
    F = dense_in.shape[1]
    share = D // Z
    De = D // E
    cap = max(2, 3 * T // (2 * E))
    C = E // 2
    away = E - 2
    others = away * cap
    nk = 2 if De == share and share % 256 == 0 else 1
    bf16 = jnp.bfloat16
    any_, vmem = pl.BlockSpec(memory_space=pl.ANY), pl.BlockSpec(memory_space=pltpu.VMEM)
    dma = pltpu.SemaphoreType.DMA
    splits = (max(1, min(8, De // (16 * G))), 8)
    subs = max(splits)
    return pl.pallas_call(
        functools.partial(kernel, G, E, Z, cap, nk, splits),
        out_shape=jax.ShapeDtypeStruct((T, share), bf16),
        in_specs=[any_, any_, any_, any_, any_, any_, any_, any_],
        out_specs=vmem,
        scratch_shapes=[
            pltpu.VMEM((D, F), bf16), pltpu.VMEM((F, D), bf16),
            pltpu.VMEM((D, F), bf16), pltpu.VMEM((F, D), bf16),
            pltpu.VMEM((T, D), bf16), pltpu.VMEM((T, D), bf16),
            pltpu.VMEM((2, others, share), bf16), pltpu.VMEM((cap, D), bf16), pltpu.VMEM((E * cap, D), bf16),
            pltpu.VMEM((max(T, 3 * cap), F), bf16),
            pltpu.VMEM((2 * cap, D), bf16), pltpu.VMEM((cap, D), bf16),
            pltpu.VMEM((Z, others, share), bf16), pltpu.VMEM((Z + 1, others, share), bf16),
            pltpu.VMEM((Z, T, share), bf16), pltpu.VMEM((Z + 1, T, share), bf16),
            pltpu.VMEM((others, share), bf16), pltpu.VMEM((others, share), bf16),
            pltpu.VMEM((T, share), jnp.float32), pltpu.VMEM((T, 2 * cap), bf16),
            pltpu.VMEM((T, 128), jnp.float32), pltpu.VMEM((T, D), bf16), pltpu.VMEM((cap, F), jnp.float32),
            pltpu.VMEM((1, T), jnp.int32), pltpu.VMEM((1, T), jnp.float32), pltpu.VMEM((1, D), jnp.float32),
            dma((12,)), dma((2,)), dma((2,)), dma((1,)), dma((1,)), dma((away, 2)), dma((away, 2)),
            dma((away, 2, Z - 1)), dma((away, 2, Z - 1)), dma((1,)), dma((1,)),
            dma((2,)), dma((2, C - 1, subs + nk * (G - 1))), dma((2,)), dma((2, C - 1, subs, G - 1)), dma((2,)), dma((1 + nk,)),
            dma((1,)), dma((away, Z + 1)), dma((1,)), dma((Z + 1, 2 * nk)), dma((away,)), dma((away,)),
        ],
        compiler_params=pltpu.CompilerParams(
            collective_id=0, has_side_effects=True, vmem_limit_bytes=67043328
        ),
    )(tokens, route.reshape(1, T), gate_prob[None, :], norm_gain[None, :], dense_in, dense_out, expert_in, expert_out)


def solution(mesh):
    return jax.shard_map(
        local,
        mesh=mesh,
        in_specs=(
            P(("groups", "expert"), None),
            P(("groups", "expert"), None),
            P(("groups", "expert")),
            P(),
            P("expert", "cuts"),
            P("cuts", "expert"),
            P("expert", None, "cuts"),
            P("expert", "cuts", None),
        ),
        out_specs=P(("groups", "expert"), "cuts"),
        check_vma=False,
    )
```
